128 devices in a mesh: grp: 4 (over y_hi, core), row: 32 (over y_lo, z, x).
Axes of the slice: x: 4, y: 4 (y_hi: 2, y_lo: 2; y = y_hi * 2 + y_lo), z: 4, core: 2. Of those that a mesh axis runs over, the one named last changes fastest.
Arguments:
- landmarks: bfloat16 [4096, 1024], P(('grp', 'row')), may hold values from -6.5 to 6.5
- initial_basis: bfloat16 [4096, 256], P(('grp', 'row')), may hold values from -0.09375 to 0.09375
- points: bfloat16 [131072, 1024], P(('grp', 'row')), may hold values from -6.5 to 6.5
Outputs:
- basis: float32 [4096, 256], P(('grp', 'row'))
- coords: float32 [131072, 256], P(('grp', 'row'))
The draws below stay inside these ranges and needn't reach their ends.
All inputs are finite; a program needn't handle non-finite values.
Results may differ from the reference program's by a relative error of at most 0.0057.
Values may be sent and summed in bfloat16 or wider, within the bound.
A program may use at most 128 MiB of HBM per device.

```python
import math
import jax
import jax.numpy as jnp
from jax import lax

D = 1024
RANK = 256
ITERS = 2
L = 4096
NP = 131072


def cluster_rows(key, salt, count):
    centers = jax.random.truncated_normal(jax.random.fold_in(key, 11), -4.0, 4.0, (64, D), jnp.float32)
    member = jax.random.randint(jax.random.fold_in(key, salt), (count,), 0, 64)
    noise = 0.6 * jax.random.truncated_normal(jax.random.fold_in(key, salt + 1), -4.0, 4.0, (count, D), jnp.float32)
    return centers[member] + noise


def draw_landmarks(key, part):
    return cluster_rows(key, 21, L).astype(jnp.bfloat16)


def draw_points(key, part):
    return cluster_rows(key, 31, NP).astype(jnp.bfloat16)


def block_scale(stream_key, dims, shards, smallest, top_value):
    def one(dim, blocks):
        heights = jax.random.uniform(jax.random.fold_in(jax.random.fold_in(stream_key, 6), dim), (blocks,), jnp.float32, smallest / len(shards), top_value / len(shards))
        return jnp.repeat(jnp.exp(heights), dims[dim] // blocks).reshape((-1,) + (1,) * (len(dims) - dim - 1))

    loudness = one(*shards[0])
    for cut in shards[1:]:
        loudness = loudness * one(*cut)
    return loudness


def bell_draw(rng, shape, scale, most, split=(), dtype=jnp.bfloat16):
    level = block_scale(rng, shape, split, -0.22, 0.18) if split else 1.0
    drawn = jax.random.normal(rng, shape, jnp.float32) * scale * level
    return jnp.minimum(jnp.maximum(drawn, -most), most).astype(dtype)


def setup_inputs(seed: int = 0) -> dict:
    key_of = jax.random.split(jax.random.key(seed), 4)
    return {
        "landmarks": draw_landmarks(jax.random.fold_in(key_of[3], 71), 0),
        "initial_basis": bell_draw(key_of[1], (L, RANK), L ** -0.5, 0.09375, ((0, 128),)),
        "points": draw_points(jax.random.fold_in(key_of[3], 71), 0),
    }


spread = 0.25

def pair_kernel(left, right):
    left_sq = lax.optimization_barrier(jnp.sum(jnp.square(left.astype(jnp.float32)), axis=1))
    right_sq = lax.optimization_barrier(jnp.sum(jnp.square(right.astype(jnp.float32)), axis=1))
    inner = lax.dot_general(left.astype(jnp.float32), right.astype(jnp.float32), (((1,), (1,)), ((), ())), precision=lax.Precision.HIGHEST)
    dist = left_sq[:, None] + right_sq[None, :] - 2.0 * inner
    return jnp.exp(-dist / (spread * left.shape[1]))

def reference(landmarks, initial_basis, points):
    total = landmarks.shape[0]
    width = landmarks.shape[1]
    blocks = landmarks.reshape(4, total // 4, width)
    land_kernel = lax.map(lambda block: pair_kernel(block, landmarks), blocks).reshape(total, total)
    degree = lax.optimization_barrier(jnp.sum(land_kernel, axis=1))
    inverse_root = 1.0 / jnp.sqrt(degree)
    affinity = (land_kernel * inverse_root[:, None] * inverse_root[None, :]).astype(jnp.bfloat16)
    affinity = lax.optimization_barrier(affinity).astype(jnp.float32)
    current = initial_basis
    for step in range(ITERS):
        image = jnp.dot(affinity, current.astype(jnp.float32), precision=lax.Precision.HIGHEST)
        gram = jnp.dot(image.T, image, precision=lax.Precision.HIGHEST)
        lower = jnp.linalg.cholesky(gram)
        ortho = jax.scipy.linalg.solve_triangular(lower, image.T, lower=True).T
        current = ortho.astype(jnp.bfloat16)
    lam = jnp.diagonal(lower)
    spectral = (ortho * inverse_root[:, None] / lam[None, :]).astype(jnp.bfloat16)
    spectral = lax.optimization_barrier(spectral).astype(jnp.float32)
    count = points.shape[0]
    block_rows = min(512, count)
    root = math.sqrt(total)

    def embed(block):
        point_kernel = pair_kernel(block, landmarks)
        point_degree = lax.optimization_barrier(jnp.sum(point_kernel, axis=1))
        weights = lax.optimization_barrier(point_kernel.astype(jnp.bfloat16)).astype(jnp.float32)
        numer = jnp.dot(weights, spectral, precision=lax.Precision.HIGHEST)
        return numer / jnp.sqrt(point_degree)[:, None] * root
    coords = lax.map(embed, points.reshape(count // block_rows, block_rows, width)).reshape(count, -1)
    return (ortho, coords)
```

```python
import functools
import math

import jax
import jax.numpy as jnp
from jax import lax
from jax.experimental import pallas as pl
from jax.experimental.pallas import tpu as pltpu
from jax.sharding import PartitionSpec as P

ITERS = 2
SPREAD = 0.25
LOG2E = 1.4426950408889634
MESH = pl.DeviceIdType.MESH
F32 = jnp.float32
BF16 = jnp.bfloat16
VMEM_LIMIT = 67_043_328


def place():
    grp, row = lax.axis_index("grp"), lax.axis_index("row")
    core, y_hi = lax.rem(grp, 2), grp // 2
    y_lo, z, x = row // 16, lax.rem(row // 4, 4), lax.rem(row, 4)
    return core, {"z": z, "y": y_hi * 2 + y_lo, "x": x}


def device(core, at):
    return ((at["y"] // 2) * 2 + core, lax.rem(at["y"], 2) * 16 + at["z"] * 4 + at["x"])


def neighbour(core, at, axis, by):
    return device(core, {**at, axis: lax.rem(at[axis] + by + 4, 4)})


def dot_nt(a, b):
    return lax.dot_general(a, b, (((1,), (1,)), ((), ())), preferred_element_type=F32)


def dot_tn(a, b):
    return lax.dot_general(a, b, (((0,), (0,)), ((), ())), preferred_element_type=F32)


ORDERS = (("x", "y", "z"), ("y", "z", "x"), ("z", "x", "y"))


def gather_kernel(
    scale, land_in, basis_in, points_ref,
    weights_out, factor_ref, land_out, basis_out, sq_out,
    land, basis, sq, wbuf, dacc,
    own_sem, send_sem, recv_sem, fsend, frecv, out_sem, w_sem,
):
    core, at = place()
    partner = device(1 - core, at)
    own = (core, at["z"], at["y"], at["x"])
    first = [
        pltpu.make_async_copy(land_in, land.at[own], own_sem.at[0]),
        pltpu.make_async_copy(basis_in, basis.at[own], own_sem.at[1]),
    ]
    for c in first:
        c.start()

    barrier = pltpu.get_barrier_semaphore()
    peers = [neighbour(core, at, a, by) for a in "xyz" for by in (1, -1)] + [partner]
    for peer in peers:
        pl.semaphore_signal(barrier, inc=1, device_id=peer, device_id_type=MESH)
    for c in first:
        c.wait()
    pl.semaphore_wait(barrier, len(peers))

    parts = (
        (land, pl.ds(0, 384), ORDERS[0]),
        (land, pl.ds(384, 384), ORDERS[1]),
        (land, pl.ds(768, 256), ORDERS[2]),
        (basis, pl.ds(0, 256), ORDERS[2]),
    )

    def block(part, phase, shift, rows=slice(None)):
        buf, cols, order = part
        index = [core]
        for a in "zyx":
            if a == order[phase]:
                index.append(lax.rem(at[a] + shift + 4, 4))
            elif a in order[:phase]:
                index.append(slice(None))
            else:
                index.append(at[a])
        return buf.at[tuple(index + [rows, cols])]

    def remote(ref, sems, index, dev):
        return pltpu.make_async_remote_copy(
            src_ref=ref, dst_ref=ref, send_sem=sems[0].at[index], recv_sem=sems[1].at[index],
            device_id=dev, device_id_type=MESH,
        )

    sent, forwarded = [], []

    def send(ref, index, dev):
        c = remote(ref, (send_sem, recv_sem), index, dev)
        c.start()
        sent.append(c)
        return c

    def forward(ref, index):
        c = remote(ref, (fsend, frecv), index, partner)
        c.start()
        forwarded.append(c)

    np_ = len(parts)
    for p, part in enumerate(parts):
        forward(block(part, 0, 0), p * 10)
    for phase in range(3):
        ring = []
        for p, part in enumerate(parts):
            a = part[2][phase]
            base = (p * 3 + phase) * 4
            up, down = neighbour(core, at, a, 1), neighbour(core, at, a, -1)
            mine = block(part, phase, 0)
            ring.append((send(mine, base, up), send(mine, base + 1, down), up, down, base))
        second = []
        for p, part in enumerate(parts):
            from_below, from_above, up, down, base = ring[p]
            from_below.wait_recv()
            far_up = send(block(part, phase, -1, pl.ds(0, 16)), base + 2, up)
            from_above.wait_recv()
            far_down = send(block(part, phase, 1, pl.ds(16, 16)), base + 3, down)
            forward(block(part, phase, -1), p * 10 + 1 + phase * 3)
            forward(block(part, phase, 1), p * 10 + 2 + phase * 3)
            second.append((far_up, far_down))
        for p, part in enumerate(parts):
            far_up, far_down = second[p]
            far_up.wait_recv()
            far_down.wait_recv()
            forward(block(part, phase, 2), p * 10 + 3 + phase * 3)
    for c in forwarded:
        c.wait_recv()

    outs = [
        pltpu.make_async_copy(land, land_out, out_sem.at[0]),
        pltpu.make_async_copy(basis, basis_out, out_sem.at[1]),
    ]
    for c in outs:
        c.start()

    def norms(b, _):
        c, z, y = b // 16, lax.rem(b // 4, 4), lax.rem(b, 4)
        rows = land[c, z, y].reshape(128, 1024).astype(F32)
        squares = rows * rows
        part = squares[:, :128]
        for k in range(1, 8):
            part += squares[:, k * 128 : (k + 1) * 128]
        line = jnp.sum(part.T, axis=0, keepdims=True) * scale
        sq[:, pl.ds(pl.multiple_of(b * 128, 128), 128)] = line
        return 0

    lax.fori_loop(0, 32, norms, 0)
    sq_copy = pltpu.make_async_copy(sq, sq_out, out_sem.at[2])
    sq_copy.start()

    tile = 256
    tiles = points_ref.shape[0] // tile
    copies = []
    for t in range(tiles):
        slot = t % 2
        if t >= 2:
            copies[t - 2].wait()
        pts = points_ref[pl.ds(t * tile, tile), :]
        wide = pts.astype(F32)
        psq = jnp.sum(wide * wide, axis=1, keepdims=True) * scale
        dacc[...] = jnp.zeros_like(dacc)

        def chunk(j, _):
            c, z = j // 4, lax.rem(j, 4)
            rows = land[c, z].reshape(512, 1024)
            cols = pl.ds(pl.multiple_of(j * 512, 512), 512)
            near = jnp.exp2(dot_nt(pts, rows) * (2.0 * scale) - (psq + sq[:, cols]))
            wbuf[slot, :, cols] = near.astype(BF16)
            dacc[...] += near[:, :128] + near[:, 128:256] + near[:, 256:384] + near[:, 384:]
            return 0

        lax.fori_loop(0, 8, chunk, 0)
        factor_ref[pl.ds(t * tile, tile), :] = 64.0 / jnp.sqrt(jnp.sum(dacc[...], axis=1, keepdims=True))
        copies.append(
            pltpu.make_async_copy(wbuf.at[slot], weights_out.at[pl.ds(t * tile, tile), :], w_sem.at[slot])
        )
        copies[-1].start()
    for c in copies[-2:]:
        c.wait()
    for c in sent:
        c.wait_send()
    for c in forwarded:
        c.wait_send()
    for c in outs:
        c.wait()
    sq_copy.wait()


def split(x):
    hi = x.astype(BF16)
    return hi, (x - hi.astype(F32)).astype(BF16)


def cholesky_inverse(aug, lower_t, inverse):
    lane = 128
    row_id = lax.broadcasted_iota(jnp.int32, (16, lane), 0)
    for b in range(16):
        r0 = b * 16
        diag = aug[pl.ds(r0, 16), :256]
        reps = [jnp.broadcast_to(diag[:, r0 + j : r0 + j + 1], (16, lane)) for j in range(16)]
        panel = [aug[pl.ds(r0, 16), pl.ds(k * lane, lane)] for k in range(4)]
        for j in range(16):
            root = lax.rsqrt(reps[j][j : j + 1, :])
            column = reps[j] * root
            for i in range(j + 1, 16):
                reps[i] = reps[i] - column * column[i : i + 1, :]
            below = jnp.where(row_id > j, column, 0.0)
            for k in range(4):
                line = panel[k][j : j + 1, :] * root
                panel[k] = jnp.where(row_id == j, line, panel[k] - below * line)
        for k in range(2):
            lower_t[pl.ds(r0, 16), pl.ds(k * lane, lane)] = panel[k]
            inverse[pl.ds(r0, 16), pl.ds(k * lane, lane)] = panel[2 + k]
        if b < 15:
            rows = jnp.concatenate(panel, axis=1)
            hi = rows.astype(BF16)
            rest = rows - hi.astype(F32)
            mid = rest.astype(BF16)
            low = (rest - mid.astype(F32)).astype(BF16)
            left = jnp.concatenate([hi, hi, mid, mid, hi, low], axis=0)[:, :256]
            right = jnp.concatenate([hi, mid, hi, mid, low, hi], axis=0)
            start = (r0 + 16) // 128 * 128
            aug[start:, :] = aug[start:, :] - dot_tn(left[:, start:], right)


def main_kernel(
    scale, land_hbm, basis_hbm, sq_ref,
    own_out, spectral_out,
    kern, xs, csum, grams, aug, lower_t, inverse, col_scale, row_scale, gacc, staged,
    in_sem, c_sem, g_sem, x_sem, s_sem, l_sem,
):
    core, at = place()
    other = 1 - core
    partner = device(other, at)
    half = kern.shape[0]
    tile, tiles = 256, half // 256
    mine = pl.multiple_of(core * half, half)

    def remote(src, dst, sems, index):
        return pltpu.make_async_remote_copy(
            src_ref=src, dst_ref=dst, send_sem=sems.at[0, index], recv_sem=sems.at[1, index],
            device_id=partner, device_id_type=MESH,
        )

    basis_in = pltpu.make_async_copy(basis_hbm, xs.at[0], in_sem.at[1])
    basis_in.start()
    barrier = pltpu.get_barrier_semaphore()
    pl.semaphore_signal(barrier, inc=1, device_id=partner, device_id_type=MESH)

    csum[0] = jnp.zeros(csum.shape[1:], F32)

    def kernel_scope(land):
        land_in = pltpu.make_async_copy(land_hbm, land, in_sem.at[0])
        land_in.start()
        land_in.wait()

        def row_tile(t, _):
            r = pl.ds(pl.multiple_of(t * tile, tile), tile)
            rows = land[pl.ds(pl.multiple_of(mine + t * tile, tile), tile), :]
            wide = rows.astype(F32)
            rsq = jnp.sum(wide * wide, axis=1, keepdims=True) * scale
            gacc[:, :128] = jnp.zeros((tile, 128), F32)

            def chunk(j, _):
                cols = pl.ds(pl.multiple_of(j * 512, 512), 512)
                near = jnp.exp2(dot_nt(rows, land[cols, :]) * (2.0 * scale) - (rsq + sq_ref[:, cols]))
                kern[r, cols] = near
                gacc[:, :128] += near[:, :128] + near[:, 128:256] + near[:, 256:384] + near[:, 384:]
                csum[0, :, cols] += jnp.sum(near.reshape(tile // 8, 8, 512), axis=0)
                return 0

            lax.fori_loop(0, 8, chunk, 0)
            col_scale[r, :] = 1.0 / jnp.sqrt(jnp.sum(gacc[:, :128], axis=1, keepdims=True))
            return 0

        lax.fori_loop(0, tiles, row_tile, 0)

    pl.run_scoped(kernel_scope, pltpu.VMEM(land_hbm.shape, BF16))
    pl.semaphore_wait(barrier, 1)
    give = remote(csum.at[0], csum.at[1], c_sem, 0)
    give.start()
    give.wait_recv()
    degree = jnp.sum(csum[0] + csum[1], axis=0, keepdims=True)
    row_scale[...] = 1.0 / jnp.sqrt(degree)
    give.wait_send()
    basis_in.wait()

    pending = []

    def iterate(affinity, image):
        eye = (
            lax.broadcasted_iota(jnp.int32, (256, 256), 0) == lax.broadcasted_iota(jnp.int32, (256, 256), 1)
        )
        for step in range(ITERS):
            gacc[...] = jnp.zeros_like(gacc)

            def image_tile(t, _):
                r = pl.ds(pl.multiple_of(t * tile, tile), tile)
                if step == 0:
                    scale_rows = col_scale[r, :]
                    for j in range(8):
                        cols = pl.ds(j * 512, 512)
                        affinity[r, cols] = (kern[r, cols] * scale_rows * row_scale[:, cols]).astype(BF16)
                img = jnp.dot(affinity[r, :], xs[step], preferred_element_type=F32)
                image[r, :] = img
                hi, lo = split(img)
                gacc[...] += dot_tn(hi, jnp.concatenate([hi, lo], axis=1))
                return 0

            lax.fori_loop(0, tiles, image_tile, 0)
            cross = gacc[:, 256:]
            grams[step, 0] = gacc[:, :256] + cross + cross.T
            swap = remote(grams.at[step, 0], grams.at[step, 1], g_sem, step)
            swap.start()
            swap.wait_recv()
            aug[:, :256] = grams[step, 0] + grams[step, 1]
            aug[:, 256:] = jnp.where(eye, 1.0, 0.0)
            swap.wait_send()
            cholesky_inverse(aug, lower_t, inverse)
            ihi, ilo = split(inverse[...])
            weights = jnp.concatenate([ihi, ilo, ihi], axis=1)
            last = step == ITERS - 1
            if last:
                lam = jnp.sum(jnp.where(eye, lower_t[...], 0.0), axis=0, keepdims=True)

            def ortho_tile(t, _):
                r = pl.ds(pl.multiple_of(t * tile, tile), tile)
                hi, lo = split(image[r, :])
                ortho = dot_nt(jnp.concatenate([hi, hi, lo], axis=1), weights)
                if last:
                    image[r, :] = ortho
                    staged[r, :] = (ortho * col_scale[r, :] / lam).astype(BF16)
                else:
                    xs[step + 1, pl.ds(pl.multiple_of(mine + t * tile, tile), tile), :] = ortho.astype(BF16)
                return 0

            lax.fori_loop(0, tiles, ortho_tile, 0)
            if last:
                give = remote(staged, spectral_out.at[pl.ds(mine, half), :], s_sem, 0)
                give.start()
                local = pltpu.make_async_copy(staged, spectral_out.at[pl.ds(mine, half), :], l_sem)
                local.start()
                index = at["z"] * 16 + at["y"] * 4 + at["x"]
                own_out[...] = image[pl.ds(pl.multiple_of(index * 32, 32), 32), :]
                local.wait()
                give.wait_recv()
                give.wait_send()
            else:
                part = xs.at[step + 1, pl.ds(mine, half), :]
                give = remote(part, part, x_sem, step)
                give.start()
                give.wait_recv()
                pending.append(give)
        for c in pending:
            c.wait_send()

    pl.run_scoped(iterate, pltpu.VMEM(kern.shape, BF16), pltpu.VMEM((half, 256), F32))


def coords_kernel(weights_ref, spectral_ref, factor_ref, out_ref):
    numer = jnp.dot(weights_ref[...], spectral_ref[...], preferred_element_type=F32)
    out_ref[...] = numer * factor_ref[...]


def body(landmarks, initial_basis, points):
    shard, width = landmarks.shape
    rank = initial_basis.shape[1]
    total = shard * 128
    half = total // 2
    count = points.shape[0]
    scale = LOG2E / (SPREAD * width)
    anywhere = pl.BlockSpec(memory_space=pl.ANY)
    vmem = pl.BlockSpec(memory_space=pltpu.VMEM)
    dma = pltpu.SemaphoreType.DMA

    weights, factor, land, basis, sq = pl.pallas_call(
        functools.partial(gather_kernel, scale),
        name="gather",
        out_shape=(
            jax.ShapeDtypeStruct((count, total), BF16),
            jax.ShapeDtypeStruct((count, 1), F32),
            jax.ShapeDtypeStruct((2, 4, 4, 4, shard, width), BF16),
            jax.ShapeDtypeStruct((2, 4, 4, 4, shard, rank), BF16),
            jax.ShapeDtypeStruct((1, total), F32),
        ),
        in_specs=[anywhere, anywhere, vmem],
        out_specs=(anywhere, vmem, anywhere, anywhere, anywhere),
        scratch_shapes=[
            pltpu.VMEM((2, 4, 4, 4, shard, width), BF16),
            pltpu.VMEM((2, 4, 4, 4, shard, rank), BF16),
            pltpu.VMEM((1, total), F32),
            pltpu.VMEM((2, 256, total), BF16),
            pltpu.VMEM((256, 128), F32),
            dma((2,)), dma((48,)), dma((48,)), dma((40,)), dma((40,)), dma((3,)), dma((2,)),
        ],
        compiler_params=pltpu.CompilerParams(
            collective_id=0, has_side_effects=True, vmem_limit_bytes=VMEM_LIMIT
        ),
    )(landmarks, initial_basis, points)

    own, spectral = pl.pallas_call(
        functools.partial(main_kernel, scale),
        name="eigenbasis",
        out_shape=(
            jax.ShapeDtypeStruct((shard, rank), F32),
            jax.ShapeDtypeStruct((total, rank), BF16),
        ),
        in_specs=[anywhere, anywhere, vmem],
        out_specs=(vmem, anywhere),
        scratch_shapes=[
            pltpu.VMEM((half, total), F32),
            pltpu.VMEM((2, total, rank), BF16),
            pltpu.VMEM((2, 8, total), F32),
            pltpu.VMEM((2, 2, rank, rank), F32),
            pltpu.VMEM((rank, 2 * rank), F32),
            pltpu.VMEM((rank, rank), F32),
            pltpu.VMEM((rank, rank), F32),
            pltpu.VMEM((half, 1), F32),
            pltpu.VMEM((1, total), F32),
            pltpu.VMEM((256, 512), F32),
            pltpu.VMEM((half, rank), BF16),
            dma((2,)), dma((2, 1)), dma((2, 2)), dma((2, 2)), dma((2, 1)), dma,
        ],
        compiler_params=pltpu.CompilerParams(
            collective_id=1, has_side_effects=True, vmem_limit_bytes=VMEM_LIMIT
        ),
    )(land.reshape(total, width), basis.reshape(total, rank), sq)

    coords = pl.pallas_call(
        coords_kernel,
        name="coords",
        grid=(count // 256,),
        out_shape=jax.ShapeDtypeStruct((count, rank), F32),
        in_specs=[
            pl.BlockSpec((256, total), lambda i: (i, 0)),
            pl.BlockSpec((total, rank), lambda i: (0, 0)),
            pl.BlockSpec((256, 1), lambda i: (i, 0)),
        ],
        out_specs=pl.BlockSpec((256, rank), lambda i: (i, 0)),
    )(weights, spectral, factor)
    return own, coords


def solution(mesh):
    in_specs = (P(("grp", "row"), None), P(("grp", "row"), None), P(("grp", "row"), None))
    out_specs = (P(("grp", "row"), None), P(("grp", "row"), None))
    return jax.shard_map(body, mesh=mesh, in_specs=in_specs, out_specs=out_specs, check_vma=False)
```

```python
import functools
import math

import jax
import jax.numpy as jnp
from jax import lax
from jax.experimental import pallas as pl
from jax.experimental.pallas import tpu as pltpu
from jax.sharding import PartitionSpec as P

ITERS = 2
SPREAD = 0.25
LOG2E = 1.4426950408889634
MESH = pl.DeviceIdType.MESH
F32 = jnp.float32
BF16 = jnp.bfloat16
VMEM_LIMIT = 67_043_328


def place():
    grp, row = lax.axis_index("grp"), lax.axis_index("row")
    core, y_hi = lax.rem(grp, 2), grp // 2
    y_lo, z, x = row // 16, lax.rem(row // 4, 4), lax.rem(row, 4)
    return core, {"z": z, "y": y_hi * 2 + y_lo, "x": x}


def device(core, at):
    return ((at["y"] // 2) * 2 + core, lax.rem(at["y"], 2) * 16 + at["z"] * 4 + at["x"])


def neighbour(core, at, axis, by):
    return device(core, {**at, axis: lax.rem(at[axis] + by + 4, 4)})


def dot_nt(a, b):
    return lax.dot_general(a, b, (((1,), (1,)), ((), ())), preferred_element_type=F32)


def dot_tn(a, b):
    return lax.dot_general(a, b, (((0,), (0,)), ((), ())), preferred_element_type=F32)


ORDERS = (("x", "y", "z"), ("y", "z", "x"), ("z", "x", "y"))


def nystrom_kernel(
    scale, land_in, basis_in, points_in,
    own_out, coords_out, weights_out,
    land, xs, norms, kern, upper, image, sq, csum, grams, aug, lower_t, inverse,
    col_scale, row_scale, factor,
    own_sem, send_sem, recv_sem, fsend, frecv, w_sem, c_sem, g_sem, x_sem, s_sem, o_sem,
):
    core, at = place()
    partner = device(1 - core, at)
    own = (core, at["z"], at["y"], at["x"])
    half = kern.shape[0]
    count = points_in.shape[0]

    first = [
        pltpu.make_async_copy(land_in, land.at[own], own_sem.at[0]),
        pltpu.make_async_copy(basis_in, xs.at[(0, *own)], own_sem.at[1]),
    ]
    for c in first:
        c.start()
    points = upper.at[:, pl.ds(0, 1024)]
    points_copy = pltpu.make_async_copy(points_in, points, own_sem.at[2])
    points_copy.start()
    barrier = pltpu.get_barrier_semaphore()
    peers = [neighbour(core, at, a, by) for a in "xyz" for by in (1, -1)] + [partner]
    for peer in peers:
        pl.semaphore_signal(barrier, inc=1, device_id=peer, device_id_type=MESH)
    for c in first:
        c.wait()
    mine = land[own].astype(F32)
    own_sq = jnp.sum(mine * mine, axis=1, keepdims=True) * scale
    lane = lax.broadcasted_iota(jnp.int32, (32, 128), 1)
    row = lax.broadcasted_iota(jnp.int32, (32, 128), 0)
    norms[own] = jnp.sum(jnp.where(lane == row + at["x"] * 32, own_sq, 0.0), axis=0, keepdims=True)
    pl.semaphore_wait(barrier, len(peers))

    everything = slice(None)
    stages = []
    for s in range(2):
        rows = pl.ds(16 * s, 16)
        stages.append([
            (land, (), rows, pl.ds(0, 384), ORDERS[0]),
            (land, (), rows, pl.ds(384, 384), ORDERS[1]),
            (land, (), rows, pl.ds(768, 256), ORDERS[2]),
            (xs, (0,), rows, pl.ds(0, 128), ORDERS[2]),
            (xs, (0,), rows, pl.ds(128, 128), ORDERS[s]),
        ])
    stages[1].append((norms, (), everything, everything, ORDERS[2]))

    def block(part, phase, shift):
        buf, lead, rows, cols, order = part
        index = [*lead, core]
        for a in "zyx":
            if a == order[phase]:
                index.append(lax.rem(at[a] + shift + 4, 4))
            elif a in order[:phase]:
                index.append(everything)
            else:
                index.append(at[a])
        return buf.at[tuple(index + [rows, cols])]

    sent, forwarded = [], []

    def send(ref, dev):
        k = len(sent)
        c = pltpu.make_async_remote_copy(
            src_ref=ref, dst_ref=ref, send_sem=send_sem.at[k], recv_sem=recv_sem.at[k],
            device_id=dev, device_id_type=MESH,
        )
        c.start()
        sent.append(c)
        return c

    def forward(ref):
        k = len(forwarded)
        c = pltpu.make_async_remote_copy(
            src_ref=ref, dst_ref=ref, send_sem=fsend.at[k], recv_sem=frecv.at[k],
            device_id=partner, device_id_type=MESH,
        )
        c.start()
        forwarded.append(c)

    def near(part, phase):
        a = part[4][phase]
        ref = block(part, phase, 0)
        return send(ref, neighbour(core, at, a, 1)), send(ref, neighbour(core, at, a, -1))

    def far(s, part, phase, arrivals):
        a = part[4][phase]
        below, above = arrivals
        if s == 0:
            below.wait_recv()
            c = send(block(part, phase, -1), neighbour(core, at, a, 1))
            above.wait_recv()
        else:
            above.wait_recv()
            c = send(block(part, phase, 1), neighbour(core, at, a, -1))
            below.wait_recv()
        forward(block(part, phase, -1))
        forward(block(part, phase, 1))
        return c

    def finish(part, phase, c):
        c.wait_recv()
        forward(block(part, phase, 2))

    far_sent = [None, None]
    for phase in range(3):
        near_sent = [None, None]
        for s, parts in enumerate(stages):
            if phase:
                for part, c in zip(parts, far_sent[s]):
                    finish(part, phase - 1, c)
            near_sent[s] = [near(part, phase) for part in parts]
            if not phase:
                for part in parts:
                    forward(block(part, 0, 0))
        for s, parts in enumerate(stages):
            far_sent[s] = [far(s, part, phase, n) for part, n in zip(parts, near_sent[s])]
    for s, parts in enumerate(stages):
        for part, c in zip(parts, far_sent[s]):
            finish(part, 2, c)
    for c in forwarded:
        c.wait_recv()

    for b in range(32):
        c, z, y = b // 16, b // 4 % 4, b % 4
        lines = norms[c, z, y]
        sq[:, b * 128 : (b + 1) * 128] = lines[0] + lines[1] + lines[2] + lines[3]

    points_copy.wait()
    wide = points[...].astype(F32)
    factor[...] = jnp.sum(wide * wide, axis=1, keepdims=True) * scale
    image[:count, 128:] = jnp.zeros((count, 128), F32)

    def weights_copy(j, slot):
        return pltpu.make_async_copy(
            upper.at[:, pl.ds(pl.multiple_of(1024 + slot * 512, 512), 512)],
            weights_out.at[:, pl.ds(pl.multiple_of(j * 512, 512), 512)],
            w_sem.at[slot],
        )

    def point_chunk(j, _):
        slot = lax.rem(j, 2)

        @pl.when(j >= 2)
        def _():
            weights_copy(j - 2, slot).wait()

        rows = land[j // 4, lax.rem(j, 4)].reshape(512, 1024)
        cols = pl.ds(pl.multiple_of(j * 512, 512), 512)
        close = jnp.exp2(dot_nt(points[...], rows) * (2.0 * scale) - (factor[...] + sq[:, cols]))
        upper[:, pl.ds(pl.multiple_of(1024 + slot * 512, 512), 512)] = close.astype(BF16)
        image[:count, 128:] += close[:, :128] + close[:, 128:256] + close[:, 256:384] + close[:, 384:]
        weights_copy(j, slot).start()
        return 0

    lax.fori_loop(0, 8, point_chunk, 0)
    factor[...] = 64.0 / jnp.sqrt(jnp.sum(image[:count, 128:], axis=1, keepdims=True))

    csum[0] = jnp.zeros(csum.shape[1:], F32)
    image[:, :128] = jnp.zeros((half, 128), F32)
    for z in range(4):
        wide = land[core, z].reshape(512, 1024).astype(F32)
        col_scale[z * 512 : (z + 1) * 512, :] = jnp.sum(wide * wide, axis=1, keepdims=True) * scale

    def land_chunk(j, _):
        rows = land[j // 8, lax.rem(j // 2, 4), pl.ds(lax.rem(j, 2) * 2, 2)].reshape(256, 1024)
        cols = pl.ds(pl.multiple_of(j * 256, 256), 256)
        inner = dot_nt(land[core].reshape(half, 1024), rows)
        close = jnp.exp2(inner * (2.0 * scale) - (col_scale[...] + sq[:, cols]))
        kern[:, cols] = close
        image[:, :128] += close[:, :128] + close[:, 128:]
        csum[0, :, cols] += jnp.sum(close.reshape(half // 8, 8, 256), axis=0)
        return 0

    lax.fori_loop(0, 16, land_chunk, 0)

    def swap(src, dst, sems, index):
        c = pltpu.make_async_remote_copy(
            src_ref=src, dst_ref=dst, send_sem=sems.at[0, index], recv_sem=sems.at[1, index],
            device_id=partner, device_id_type=MESH,
        )
        c.start()
        return c

    give = swap(csum.at[0], csum.at[1], c_sem, 0)
    col_scale[...] = 1.0 / jnp.sqrt(jnp.sum(image[:, :128], axis=1, keepdims=True))
    give.wait_recv()
    row_scale[...] = 1.0 / jnp.sqrt(jnp.sum(csum[0] + csum[1], axis=0, keepdims=True))
    weights_copy(6, 0).wait()
    weights_copy(7, 1).wait()
    for c in sent:
        c.wait_send()
    for c in forwarded:
        c.wait_send()
    give.wait_send()

    eye = lax.broadcasted_iota(jnp.int32, (256, 256), 0) == lax.broadcasted_iota(jnp.int32, (256, 256), 1)
    pending = []
    for step in range(ITERS):
        last = step == ITERS - 1

        def lower_tile(t, _):
            r = pl.ds(pl.multiple_of(t * 512, 512), 512)
            pieces = []
            for c in range(4):
                place_at = (c // 2, c % 2 * 2 + t)
                if step == 0:
                    cols = pl.ds(c * 1024, 1024)
                    piece = (kern[r, cols] * col_scale[r, :] * row_scale[:, cols]).astype(BF16)
                    land[place_at] = piece.reshape(4, 4, 32, 1024)
                pieces.append(land[place_at].reshape(512, 1024))
            rows = jnp.concatenate(pieces, axis=1)
            image[r, :] = jnp.dot(rows, xs[step].reshape(2 * half, 256), preferred_element_type=F32)
            return 0

        def upper_tile(t, _):
            r = pl.ds(pl.multiple_of(1024 + t * 512, 512), 512)
            u = pl.ds(pl.multiple_of(t * 512, 512), 512)
            if step == 0:
                for c in range(4):
                    cols = pl.ds(c * 1024, 1024)
                    upper[u, cols] = (kern[r, cols] * col_scale[r, :] * row_scale[:, cols]).astype(BF16)
            image[r, :] = jnp.dot(upper[u, :], xs[step].reshape(2 * half, 256), preferred_element_type=F32)
            return 0

        lax.fori_loop(0, 2, upper_tile, 0)
        if last:
            weights_in = pltpu.make_async_copy(weights_out, upper, w_sem.at[0])
            weights_in.start()
        lax.fori_loop(0, 2, lower_tile, 0)
        hi, lo = split(image[...])
        gram = dot_tn(hi, jnp.concatenate([hi, lo], axis=1))
        cross = gram[:, 256:]
        grams[step, 0] = gram[:, :256] + cross + cross.T
        give = swap(grams.at[step, 0], grams.at[step, 1], g_sem, step)
        aug[:, 256:] = jnp.where(eye, 1.0, 0.0)
        give.wait_recv()
        aug[:, :256] = grams[step, 0] + grams[step, 1]
        pending.append(give)
        cholesky_inverse(aug, lower_t, inverse)
        ihi, ilo = split(inverse[...])
        stacked = jnp.concatenate([ihi, ilo, ihi], axis=1)
        if last:
            inverse_lam = 1.0 / jnp.sum(jnp.where(eye, lower_t[...], 0.0), axis=0, keepdims=True)
        gives = []
        target = 0 if last else step + 1
        for t in range(2):
            r = pl.ds(t * 1024, 1024)
            hi, lo = split(image[r, :])
            ortho = dot_nt(jnp.concatenate([hi, hi, lo], axis=1), stacked)
            if last:
                image[r, :] = ortho
                ortho = ortho * col_scale[r, :] * inverse_lam
            xs[target, core, 2 * t : 2 * t + 2] = ortho.astype(BF16).reshape(2, 4, 4, 32, 256)
            part = xs.at[target, core, pl.ds(2 * t, 2)]
            gives.append(swap(part, part, s_sem if last else x_sem, t))
        if last:
            index = at["z"] * 16 + at["y"] * 4 + at["x"]
            own_out[...] = image[pl.ds(pl.multiple_of(index * 32, 32), 32), :]
            weights_in.wait()
        for c in gives:
            c.wait_recv()
        pending += gives

    copies = []
    for t in range(2):
        r = pl.ds(t * 512, 512)
        numer = jnp.dot(upper[r, :], xs[0].reshape(2 * half, 256), preferred_element_type=F32)
        image[r, :] = numer * factor[r, :]
        copies.append(pltpu.make_async_copy(image.at[r, :], coords_out.at[r, :], o_sem.at[t]))
        copies[-1].start()
    for c in pending:
        c.wait_send()
    for c in copies:
        c.wait()


def split(x):
    hi = x.astype(BF16)
    return hi, (x - hi.astype(F32)).astype(BF16)


def cholesky_inverse(aug, lower_t, inverse):
    lane = 128
    row_id = lax.broadcasted_iota(jnp.int32, (16, lane), 0)
    for b in range(16):
        r0 = b * 16
        diag = aug[pl.ds(r0, 16), :256]
        reps = [jnp.broadcast_to(diag[:, r0 + j : r0 + j + 1], (16, lane)) for j in range(16)]
        panel = [aug[pl.ds(r0, 16), pl.ds(k * lane, lane)] for k in range(4)]
        for j in range(16):
            root = lax.rsqrt(reps[j][j : j + 1, :])
            column = reps[j] * root
            for i in range(j + 1, 16):
                reps[i] = reps[i] - column * column[i : i + 1, :]
            below = jnp.where(row_id > j, column, 0.0)
            for k in range(4):
                line = panel[k][j : j + 1, :] * root
                panel[k] = jnp.where(row_id == j, line, panel[k] - below * line)
        for k in range(2):
            lower_t[pl.ds(r0, 16), pl.ds(k * lane, lane)] = panel[k]
            inverse[pl.ds(r0, 16), pl.ds(k * lane, lane)] = panel[2 + k]
        if b < 15:
            rows = jnp.concatenate(panel, axis=1)
            hi = rows.astype(BF16)
            rest = rows - hi.astype(F32)
            mid = rest.astype(BF16)
            low = (rest - mid.astype(F32)).astype(BF16)
            left = jnp.concatenate([hi, hi, mid, mid, hi, low], axis=0)[:, :256]
            right = jnp.concatenate([hi, mid, hi, mid, low, hi], axis=0)
            start = (r0 + 16) // 128 * 128
            aug[start:, :] = aug[start:, :] - dot_tn(left[:, start:], right)


def body(landmarks, initial_basis, points):
    shard, width = landmarks.shape
    rank = initial_basis.shape[1]
    total = shard * 128
    half = total // 2
    count = points.shape[0]
    scale = LOG2E / (SPREAD * width)
    anywhere = pl.BlockSpec(memory_space=pl.ANY)
    vmem = pl.BlockSpec(memory_space=pltpu.VMEM)
    dma = pltpu.SemaphoreType.DMA

    own, coords, _ = pl.pallas_call(
        functools.partial(nystrom_kernel, scale),
        name="nystrom",
        out_shape=(
            jax.ShapeDtypeStruct((shard, rank), F32),
            jax.ShapeDtypeStruct((count, rank), F32),
            jax.ShapeDtypeStruct((count, total), BF16),
        ),
        in_specs=[anywhere, anywhere, anywhere],
        out_specs=(vmem, anywhere, anywhere),
        scratch_shapes=[
            pltpu.VMEM((2, 4, 4, 4, shard, width), BF16),
            pltpu.VMEM((2, 2, 4, 4, 4, shard, rank), BF16),
            pltpu.VMEM((2, 4, 4, 4, 1, 128), F32),
            pltpu.VMEM((half, total), F32),
            pltpu.VMEM((count, total), BF16),
            pltpu.VMEM((half, rank), F32),
            pltpu.VMEM((1, total), F32),
            pltpu.VMEM((2, 8, total), F32),
            pltpu.VMEM((2, 2, rank, rank), F32),
            pltpu.VMEM((rank, 2 * rank), F32),
            pltpu.VMEM((rank, rank), F32),
            pltpu.VMEM((rank, rank), F32),
            pltpu.VMEM((half, 1), F32),
            pltpu.VMEM((1, total), F32),
            pltpu.VMEM((count, 1), F32),
            dma((3,)), dma((99,)), dma((99,)), dma((110,)), dma((110,)), dma((2,)),
            dma((2, 1)), dma((2, 2)), dma((2, 2)), dma((2, 2)), dma((2,)),
        ],
        compiler_params=pltpu.CompilerParams(
            collective_id=0, has_side_effects=True, vmem_limit_bytes=VMEM_LIMIT
        ),
    )(landmarks, initial_basis, points)
    return own, coords


def solution(mesh):
    in_specs = (P(("grp", "row"), None), P(("grp", "row"), None), P(("grp", "row"), None))
    out_specs = (P(("grp", "row"), None), P(("grp", "row"), None))
    return jax.shard_map(body, mesh=mesh, in_specs=in_specs, out_specs=out_specs, check_vma=False)
```

```python
import functools
import math

import jax
import jax.numpy as jnp
from jax import lax
from jax.experimental import pallas as pl
from jax.experimental.pallas import tpu as pltpu
from jax.sharding import PartitionSpec as P

ITERS = 2
SPREAD = 0.25
LOG2E = 1.4426950408889634
MESH = pl.DeviceIdType.MESH
F32 = jnp.float32
BF16 = jnp.bfloat16
VMEM_LIMIT = 67_043_328


def place():
    grp, row = lax.axis_index("grp"), lax.axis_index("row")
    core, y_hi = lax.rem(grp, 2), grp // 2
    y_lo, z, x = row // 16, lax.rem(row // 4, 4), lax.rem(row, 4)
    return core, {"z": z, "y": y_hi * 2 + y_lo, "x": x}


def device(core, at):
    return ((at["y"] // 2) * 2 + core, lax.rem(at["y"], 2) * 16 + at["z"] * 4 + at["x"])


def neighbour(core, at, axis, by):
    return device(core, {**at, axis: lax.rem(at[axis] + by + 4, 4)})


def dot_nt(a, b):
    return lax.dot_general(a, b, (((1,), (1,)), ((), ())), preferred_element_type=F32)


def dot_tn(a, b):
    return lax.dot_general(a, b, (((0,), (0,)), ((), ())), preferred_element_type=F32)


ORDERS = (("x", "y", "z"), ("y", "z", "x"), ("z", "x", "y"))
EVERY = slice(None)


def split(x):
    hi = x.astype(BF16)
    return hi, (x - hi.astype(F32)).astype(BF16)


def in_three(x):
    hi = x.astype(BF16)
    rest = x - hi.astype(F32)
    mid = rest.astype(BF16)
    return hi, mid, (rest - mid.astype(F32)).astype(BF16)


def cholesky_inverse(aug, lower_t, inverse):
    lane, size = 128, 32
    row_id = lax.broadcasted_iota(jnp.int32, (size, lane), 0)
    for r0 in range(0, 256, size):
        end = r0 + size
        diag = aug[pl.ds(r0, size), :256]
        reps = [jnp.broadcast_to(diag[:, r0 + j : r0 + j + 1], (size, lane)) for j in range(size)]
        panel = [aug[pl.ds(r0, size), pl.ds(k * lane, lane)] for k in range(4)]
        live = [k for k in range(4) if (k < 2 and (k + 1) * lane > r0) or (k >= 2 and (k - 2) * lane < end)]
        for j in range(size):
            root = lax.rsqrt(reps[j][j : j + 1, :])
            column = reps[j] * root
            for i in range(j + 1, size):
                reps[i] = reps[i] - column * column[i : i + 1, :]
            below = jnp.where(row_id > j, column, 0.0)
            for k in live:
                line = panel[k][j : j + 1, :] * root
                panel[k] = jnp.where(row_id == j, line, panel[k] - below * line)
        for k in range(2):
            lower_t[pl.ds(r0, size), pl.ds(k * lane, lane)] = panel[k]
            inverse[pl.ds(r0, size), pl.ds(k * lane, lane)] = panel[2 + k]
        if end < 256:
            start = end // lane * lane
            after = [k for k in range(4) if (k < 2 and k * lane >= start) or (k >= 2 and (k - 2) * lane < end)]
            terms = [in_three(panel[k]) for k in range(4)]

            def stack(columns, order):
                return jnp.concatenate(
                    [jnp.concatenate([terms[k][o] for o in order], axis=0) for k in columns], axis=1
                )

            left = stack(range(start // lane, 2), (0, 0, 1, 1, 0, 2))
            change = dot_tn(left, stack(after, (0, 1, 0, 1, 2, 0)))
            for n, k in enumerate(after):
                cols = pl.ds(k * lane, lane)
                aug[start:, cols] = aug[start:, cols] - change[:, n * lane : (n + 1) * lane]


def nystrom_kernel(
    scale, land_in, basis_in, points_in,
    own_out, coords_out, weights_out,
    land, xs, norms, kern, upper, image, sq, csum, grams, aug, lower_t, inverse,
    col_scale, row_scale, factor,
    own_sem, send_sem, recv_sem, fsend, frecv, w_sem, c_sem, g_sem, x_sem, s_sem, o_sem,
):
    core, at = place()
    partner = device(1 - core, at)
    own = (core, at["z"], at["y"], at["x"])
    half = kern.shape[0]
    count = points_in.shape[0]

    first = []
    for s in range(2):
        rows = pl.ds(16 * s, 16)
        first.append(pltpu.make_async_copy(land_in.at[rows, :], land.at[(s, *own)], own_sem.at[s]))
        first.append(pltpu.make_async_copy(basis_in.at[rows, :], xs.at[(0, s, *own)], own_sem.at[2 + s]))
    for c in first:
        c.start()
    points = upper.at[:, pl.ds(0, 1024)]
    points_copy = pltpu.make_async_copy(points_in, points, own_sem.at[4])
    points_copy.start()
    barrier = pltpu.get_barrier_semaphore()
    peers = [neighbour(core, at, a, by) for a in "xyz" for by in (1, -1, 2)] + [partner]
    for peer in peers:
        pl.semaphore_signal(barrier, inc=1, device_id=peer, device_id_type=MESH)
    for c in first:
        c.wait()
    offset = lax.rem(at["y"], 2) * 64 + at["x"] * 16
    spot = lax.broadcasted_iota(jnp.int32, (16, 128), 1) == lax.broadcasted_iota(jnp.int32, (16, 128), 0) + offset
    lines = []
    for s in range(2):
        mine = land[(s, *own)].astype(F32)
        own_sq = jnp.sum(mine * mine, axis=1, keepdims=True) * scale
        lines.append(jnp.sum(jnp.where(spot, own_sq, 0.0), axis=0, keepdims=True))
    norms[own] = jnp.concatenate(lines, axis=0)
    pl.semaphore_wait(barrier, len(peers))

    stages = []
    for s in range(2):
        stages.append([
            (land, (s,), pl.ds(0, 384), ORDERS[0]),
            (land, (s,), pl.ds(384, 384), ORDERS[1]),
            (land, (s,), pl.ds(768, 256), ORDERS[2]),
        ])
    stages[0].append((norms, (), EVERY, ORDERS[2]))
    late = [(xs, (0, 0), EVERY, ORDERS[0]), (xs, (0, 1), EVERY, ORDERS[1])]

    def block(part, phase, shift):
        buf, lead, cols, order = part
        index = [*lead, core]
        for a in "zyx":
            if a == order[phase]:
                index.append(lax.rem(at[a] + shift + 4, 4))
            elif a in order[:phase]:
                index.append(EVERY)
            else:
                index.append(at[a])
        return buf.at[tuple(index + [EVERY, cols])]

    sent, forwarded = [], []

    def send(part, phase, shift, by):
        k = len(sent)
        ref = block(part, phase, shift)
        c = pltpu.make_async_remote_copy(
            src_ref=ref, dst_ref=ref, send_sem=send_sem.at[k], recv_sem=recv_sem.at[k],
            device_id=neighbour(core, at, part[3][phase], by), device_id_type=MESH,
        )
        c.start()
        sent.append(c)
        return c

    def forward(part, phase, shift):
        k = len(forwarded)
        ref = block(part, phase, shift)
        c = pltpu.make_async_remote_copy(
            src_ref=ref, dst_ref=ref, send_sem=fsend.at[k], recv_sem=frecv.at[k],
            device_id=partner, device_id_type=MESH,
        )
        c.start()
        forwarded.append(c)
        return c

    def around(parts, phase):
        return [send(part, phase, 0, by) for by in (2, 1, -1) for part in parts]

    def receive(copies):
        for c in copies:
            c.wait_recv()

    ring = [around(parts, 0) for parts in stages]
    points_copy.wait()
    wide = points[...].astype(F32)
    factor[...] = jnp.sum(wide * wide, axis=1, keepdims=True) * scale
    image[...] = jnp.zeros_like(image)
    csum[0] = jnp.zeros(csum.shape[1:], F32)
    for s, parts in enumerate(stages):
        receive(ring[s])
        ring[s] = around(parts, 1)
    here, there = stages
    handed = [[], []]
    receive(ring[0])
    here_up = [send(part, 2, 0, 1) for part in here]
    here_down = [send(part, 2, 0, -1) for part in here]
    handed[0] += [forward(part, 2, 0) for part in here]
    receive(ring[1])
    there_down = [send(part, 2, 0, -1) for part in there]
    handed[1] += [forward(part, 2, 0) for part in there]
    here_far = []
    for part, c in zip(here, here_up):
        c.wait_recv()
        here_far.append(send(part, 2, -1, 1))
    there_up = [send(part, 2, 0, 1) for part in there]
    handed[0] += [forward(part, 2, -1) for part in here]
    receive(here_down)
    handed[0] += [forward(part, 2, 1) for part in here]
    there_far = []
    for part, c in zip(there, there_down):
        c.wait_recv()
        there_far.append(send(part, 2, 1, -1))
    handed[1] += [forward(part, 2, 1) for part in there]
    for part, c in zip(here, here_far):
        c.wait_recv()
        handed[0].append(forward(part, 2, 2))
    late_ring = around(late, 0)

    def own_norms(s):
        wide = land[s, core].reshape(half // 2, 1024).astype(F32)
        rows = pl.ds(s * (half // 2), half // 2)
        col_scale[rows, :] = jnp.sum(wide * wide, axis=1, keepdims=True) * scale

    own_norms(0)
    receive(handed[0])
    for c in range(2):
        for z in range(4):
            for pair in range(2):
                lines = norms[c, z, 2 * pair, 0]
                for a, x in [(0, 1), (0, 2), (0, 3), (1, 0), (1, 1), (1, 2), (1, 3)]:
                    lines += norms[c, z, 2 * pair + a, x]
                q = (c * 8 + z * 2 + pair) * 128
                sq[:, q : q + 128] = lines[0:1]
                sq[:, half + q : half + q + 128] = lines[1:2]

    def weights_copy(j, slot):
        return pltpu.make_async_copy(
            upper.at[:, pl.ds(pl.multiple_of(1024 + slot * 512, 512), 512)],
            weights_out.at[:, pl.ds(pl.multiple_of(j * 512, 512), 512)],
            w_sem.at[slot],
        )

    def point_chunk(j, _):
        slot = lax.rem(j, 2)

        @pl.when(j >= 2)
        def _():
            weights_copy(j - 2, slot).wait()

        rows = land[j // 4, lax.rem(j // 2, 2), pl.ds(lax.rem(j, 2) * 2, 2)].reshape(512, 1024)
        cols = pl.ds(pl.multiple_of(j * 512, 512), 512)
        close = jnp.exp2(dot_nt(points[...], rows) * (2.0 * scale) - (factor[...] + sq[:, cols]))
        upper[:, pl.ds(pl.multiple_of(1024 + slot * 512, 512), 512)] = close.astype(BF16)
        image[:count, 128:] += close[:, :128] + close[:, 128:256] + close[:, 256:384] + close[:, 384:]
        weights_copy(j, slot).start()
        return 0

    lax.fori_loop(0, 2, point_chunk, 0)
    for part, c, u in zip(there, there_far, there_up):
        u.wait_recv()
        handed[1].append(forward(part, 2, -1))
        c.wait_recv()
        handed[1].append(forward(part, 2, 2))
    receive(late_ring)
    late_ring = around(late, 1)
    own_norms(1)
    lax.fori_loop(2, 4, point_chunk, 0)
    receive(handed[1])
    lax.fori_loop(4, 8, point_chunk, 0)
    factor[...] = 64.0 / jnp.sqrt(jnp.sum(image[:count, 128:], axis=1, keepdims=True))
    receive(late_ring)
    late_up = [send(part, 2, 0, 1) for part in late]
    late_down = [send(part, 2, 0, -1) for part in late]
    late_handed = [forward(part, 2, 0) for part in late]

    def land_chunk(j, _):
        rows = land[j // 8, lax.rem(j // 4, 2), lax.rem(j, 4)].reshape(256, 1024)
        cols = pl.ds(pl.multiple_of(j * 256, 256), 256)
        inner = dot_nt(land[:, core].reshape(half, 1024), rows)
        close = jnp.exp2(inner * (2.0 * scale) - (col_scale[...] + sq[:, cols]))
        kern[:, cols] = close
        image[:, :128] += close[:, :128] + close[:, 128:]
        csum[0, :, cols] += jnp.sum(close.reshape(half // 8, 8, 256), axis=0)
        return 0

    lax.fori_loop(0, 6, land_chunk, 0)
    receive(late_up + late_down)
    late_far = [send(late[0], 2, -1, 1), send(late[1], 2, 1, -1)]
    late_handed += [forward(part, 2, by) for part in late for by in (-1, 1)]
    lax.fori_loop(6, 12, land_chunk, 0)
    receive(late_far)
    late_handed += [forward(part, 2, 2) for part in late]
    lax.fori_loop(12, 16, land_chunk, 0)

    def swap(src, dst, sems, index):
        c = pltpu.make_async_remote_copy(
            src_ref=src, dst_ref=dst, send_sem=sems.at[0, index], recv_sem=sems.at[1, index],
            device_id=partner, device_id_type=MESH,
        )
        c.start()
        return c

    give = swap(csum.at[0], csum.at[1], c_sem, 0)
    col_scale[...] = 1.0 / jnp.sqrt(jnp.sum(image[:, :128], axis=1, keepdims=True))
    weights_copy(6, 0).wait()
    weights_copy(7, 1).wait()
    receive(late_handed)
    for c in sent + forwarded:
        c.wait_send()
    give.wait_recv()
    row_scale[...] = 1.0 / jnp.sqrt(jnp.sum(csum[0] + csum[1], axis=0, keepdims=True))
    give.wait_send()

    def low_piece(t, s, c):
        return land[s, c, pl.ds(2 * t, 2)].reshape(512, 1024)

    def up_piece(t, s, c):
        cols = pl.ds(pl.multiple_of(s * 2048 + c * 1024, 1024), 1024)
        return upper[pl.ds(pl.multiple_of(t * 512, 512), 512), cols]

    def half_product(piece, t, slot, c):
        rows = jnp.concatenate([piece(t, 0, c), piece(t, 1, c)], axis=1)
        return jnp.dot(rows, xs[slot, :, c].reshape(half, 256), preferred_element_type=F32)

    def scaled(r, b):
        cols = pl.ds(b * 1024, 1024)
        return (kern[r, cols] * col_scale[r, :] * row_scale[:, cols]).astype(BF16)

    def first_low(t, _):
        r = pl.ds(pl.multiple_of(t * 512, 512), 512)
        pieces = []
        for b in range(4):
            piece = scaled(r, b)
            land[b // 2, b % 2, pl.ds(2 * t, 2)] = piece.reshape(2, 4, 4, 16, 1024)
            pieces.append(piece)
        rows = jnp.concatenate(pieces, axis=1)
        image[r, :] = jnp.dot(rows, xs[0].reshape(2 * half, 256), preferred_element_type=F32)
        return 0

    def first_up(t, _):
        r = pl.ds(pl.multiple_of(1024 + t * 512, 512), 512)
        u = pl.ds(pl.multiple_of(t * 512, 512), 512)
        for b in range(4):
            upper[u, pl.ds(b * 1024, 1024)] = scaled(r, b)
        image[r, :] = jnp.dot(upper[u, :], xs[0].reshape(2 * half, 256), preferred_element_type=F32)
        return 0

    eye = lax.broadcasted_iota(jnp.int32, (256, 256), 0) == lax.broadcasted_iota(jnp.int32, (256, 256), 1)
    pending, gives = [], []
    for step in range(ITERS):
        last = step == ITERS - 1
        if step == 0:
            lax.fori_loop(0, 2, first_low, 0)
            lax.fori_loop(0, 2, first_up, 0)
        else:
            def product(piece, base, c, add):
                def tile(t, _):
                    r = pl.ds(pl.multiple_of(base + t * 512, 512), 512)
                    out = half_product(piece, t, step, c)
                    image[r, :] = image[r, :] + out if add else out
                    return 0

                lax.fori_loop(0, 2, tile, 0)

            product(low_piece, 0, core, False)
            product(up_piece, 1024, core, False)
            receive(gives)
            product(up_piece, 1024, 1 - core, True)
            if last:
                weights_in = pltpu.make_async_copy(weights_out, upper, w_sem.at[0])
                weights_in.start()
            product(low_piece, 0, 1 - core, True)
        hi, lo = split(image[...])
        gram = dot_tn(hi, jnp.concatenate([hi, lo], axis=1))
        cross = gram[:, 256:]
        grams[step, 0] = gram[:, :256] + cross + cross.T
        give = swap(grams.at[step, 0], grams.at[step, 1], g_sem, step)
        aug[:, 256:] = jnp.where(eye, 1.0, 0.0)
        give.wait_recv()
        aug[:, :256] = grams[step, 0] + grams[step, 1]
        pending.append(give)
        cholesky_inverse(aug, lower_t, inverse)
        ihi, ilo = split(inverse[...])
        stacked = jnp.concatenate([ihi, ilo, ihi], axis=1)
        if last:
            inverse_lam = 1.0 / jnp.sum(jnp.where(eye, lower_t[...], 0.0), axis=0, keepdims=True)
        gives = []
        target = 0 if last else step + 1
        for t in range(2):
            r = pl.ds(t * 1024, 1024)
            hi, lo = split(image[r, :])
            ortho = dot_nt(jnp.concatenate([hi, hi, lo], axis=1), stacked)
            if last:
                image[r, :] = ortho
                ortho = ortho * col_scale[r, :] * inverse_lam
            xs[target, t, core] = ortho.astype(BF16).reshape(4, 4, 4, 16, 256)
            part = xs.at[target, t, core]
            gives.append(swap(part, part, s_sem if last else x_sem, t))
        pending += gives

    index = at["z"] * 16 + at["y"] * 4 + at["x"]
    for s in range(2):
        rows = pl.ds(pl.multiple_of(s * 1024 + index * 16, 16), 16)
        own_out[16 * s : 16 * s + 16, :] = image[rows, :]
    weights_in.wait()
    for t in range(2):
        image[t * 512 : t * 512 + 512, :] = half_product(up_piece, t, 0, core)
    receive(gives)
    copies = []
    for t in range(2):
        r = pl.ds(t * 512, 512)
        image[r, :] = (image[r, :] + half_product(up_piece, t, 0, 1 - core)) * factor[r, :]
        copies.append(pltpu.make_async_copy(image.at[r, :], coords_out.at[r, :], o_sem.at[t]))
        copies[-1].start()
    for c in pending:
        c.wait_send()
    for c in copies:
        c.wait()


def deliver_kernel(own_ref, coords_ref, own_out, coords_out):
    own_out[...] = own_ref[...]
    coords_out[...] = coords_ref[...]


def body(landmarks, initial_basis, points):
    shard, width = landmarks.shape
    rank = initial_basis.shape[1]
    total = shard * 128
    half = total // 2
    count = points.shape[0]
    scale = LOG2E / (SPREAD * width)
    anywhere = pl.BlockSpec(memory_space=pl.ANY)
    vmem = pl.BlockSpec(memory_space=pltpu.VMEM)
    dma = pltpu.SemaphoreType.DMA
    results = (jax.ShapeDtypeStruct((shard, rank), F32), jax.ShapeDtypeStruct((count, rank), F32))

    own, coords, _ = pl.pallas_call(
        functools.partial(nystrom_kernel, scale),
        name="nystrom",
        out_shape=(*results, jax.ShapeDtypeStruct((count, total), BF16)),
        in_specs=[anywhere, anywhere, anywhere],
        out_specs=(vmem, anywhere, anywhere),
        scratch_shapes=[
            pltpu.VMEM((2, 2, 4, 4, 4, shard // 2, width), BF16),
            pltpu.VMEM((2, 2, 2, 4, 4, 4, shard // 2, rank), BF16),
            pltpu.VMEM((2, 4, 4, 4, 2, 128), F32),
            pltpu.VMEM((half, total), F32),
            pltpu.VMEM((count, total), BF16),
            pltpu.VMEM((half, rank), F32),
            pltpu.VMEM((1, total), F32),
            pltpu.VMEM((2, 8, total), F32),
            pltpu.VMEM((2, 2, rank, rank), F32),
            pltpu.VMEM((rank, 2 * rank), F32),
            pltpu.VMEM((rank, rank), F32),
            pltpu.VMEM((rank, rank), F32),
            pltpu.VMEM((half, 1), F32),
            pltpu.VMEM((1, total), F32),
            pltpu.VMEM((count, 1), F32),
            dma((5,)), dma((81,)), dma((81,)), dma((36,)), dma((36,)), dma((2,)),
            dma((2, 1)), dma((2, 2)), dma((2, 2)), dma((2, 2)), dma((2,)),
        ],
        compiler_params=pltpu.CompilerParams(
            collective_id=0, has_side_effects=True, vmem_limit_bytes=VMEM_LIMIT
        ),
    )(landmarks, initial_basis, points)
    return pl.pallas_call(
        deliver_kernel,
        name="deliver",
        out_shape=results,
        in_specs=[vmem, vmem],
        out_specs=(vmem, vmem),
    )(own, coords)


def solution(mesh):
    in_specs = (P(("grp", "row"), None), P(("grp", "row"), None), P(("grp", "row"), None))
    out_specs = (P(("grp", "row"), None), P(("grp", "row"), None))
    return jax.shard_map(body, mesh=mesh, in_specs=in_specs, out_specs=out_specs, check_vma=False)
```

```python
import functools
import math

import jax
import jax.numpy as jnp
from jax import lax
from jax.experimental import pallas as pl
from jax.experimental.pallas import tpu as pltpu
from jax.sharding import PartitionSpec as P

ITERS = 2
SPREAD = 0.25
LOG2E = 1.4426950408889634
MESH = pl.DeviceIdType.MESH
F32 = jnp.float32
BF16 = jnp.bfloat16
VMEM_LIMIT = 67_043_328


def place():
    grp, row = lax.axis_index("grp"), lax.axis_index("row")
    core, y_hi = lax.rem(grp, 2), grp // 2
    y_lo, z, x = row // 16, lax.rem(row // 4, 4), lax.rem(row, 4)
    return core, {"z": z, "y": y_hi * 2 + y_lo, "x": x}


def device(core, at):
    return ((at["y"] // 2) * 2 + core, lax.rem(at["y"], 2) * 16 + at["z"] * 4 + at["x"])


def neighbour(core, at, axis, by):
    return device(core, {**at, axis: lax.rem(at[axis] + by + 4, 4)})


def dot_nt(a, b):
    return lax.dot_general(a, b, (((1,), (1,)), ((), ())), preferred_element_type=F32)


def dot_tn(a, b):
    return lax.dot_general(a, b, (((0,), (0,)), ((), ())), preferred_element_type=F32)


ORDERS = (("x", "y", "z"), ("y", "z", "x"), ("z", "x", "y"))
EVERY = slice(None)


def split(x):
    hi = x.astype(BF16)
    return hi, (x - hi.astype(F32)).astype(BF16)


def in_three(x):
    hi = x.astype(BF16)
    rest = x - hi.astype(F32)
    mid = rest.astype(BF16)
    return hi, mid, (rest - mid.astype(F32)).astype(BF16)


def cholesky_inverse(aug, lower_t, inverse):
    lane, size = 128, 32
    row_id = lax.broadcasted_iota(jnp.int32, (size, lane), 0)
    for r0 in range(0, 256, size):
        end = r0 + size
        diag = aug[pl.ds(r0, size), :256]
        reps = [jnp.broadcast_to(diag[:, r0 + j : r0 + j + 1], (size, lane)) for j in range(size)]
        panel = [aug[pl.ds(r0, size), pl.ds(k * lane, lane)] for k in range(4)]
        live = [k for k in range(4) if (k < 2 and (k + 1) * lane > r0) or (k >= 2 and (k - 2) * lane < end)]
        for j in range(size):
            root = lax.rsqrt(reps[j][j : j + 1, :])
            column = reps[j] * root
            for i in range(j + 1, size):
                reps[i] = reps[i] - column * column[i : i + 1, :]
            below = jnp.where(row_id > j, column, 0.0)
            for k in live:
                line = panel[k][j : j + 1, :] * root
                panel[k] = jnp.where(row_id == j, line, panel[k] - below * line)
        for k in range(2):
            lower_t[pl.ds(r0, size), pl.ds(k * lane, lane)] = panel[k]
            inverse[pl.ds(r0, size), pl.ds(k * lane, lane)] = panel[2 + k]
        if end < 256:
            start = end // lane * lane
            after = [k for k in range(4) if (k < 2 and k * lane >= start) or (k >= 2 and (k - 2) * lane < end)]
            terms = [in_three(panel[k]) for k in range(4)]

            def stack(columns, order):
                return jnp.concatenate(
                    [jnp.concatenate([terms[k][o] for o in order], axis=0) for k in columns], axis=1
                )

            left = stack(range(start // lane, 2), (0, 0, 1, 1, 0, 2))
            change = dot_tn(left, stack(after, (0, 1, 0, 1, 2, 0)))
            for n, k in enumerate(after):
                cols = pl.ds(k * lane, lane)
                aug[start:, cols] = aug[start:, cols] - change[:, n * lane : (n + 1) * lane]


def nystrom_kernel(
    scale, land_in, basis_in, points_in,
    own_out, coords_out, weights_out,
    land, xs, norms, kern, upper, image, sq, csum, grams, aug, lower_t, inverse,
    col_scale, row_scale, factor,
    own_sem, send_sem, recv_sem, fsend, frecv, w_sem, c_sem, g_sem, x_sem, s_sem, o_sem,
):
    core, at = place()
    partner = device(1 - core, at)
    own = (core, at["z"], at["y"], at["x"])
    half = kern.shape[0]
    count = points_in.shape[0]

    first = []
    for s in range(2):
        rows = pl.ds(16 * s, 16)
        first.append(pltpu.make_async_copy(land_in.at[rows, :], land.at[(s, *own)], own_sem.at[s]))
        first.append(pltpu.make_async_copy(basis_in.at[rows, :], xs.at[(0, s, *own)], own_sem.at[2 + s]))
    for c in first:
        c.start()
    points = upper.at[:, pl.ds(0, 1024)]
    points_copy = pltpu.make_async_copy(points_in, points, own_sem.at[4])
    points_copy.start()
    barrier = pltpu.get_barrier_semaphore()
    peers = [neighbour(core, at, a, by) for a in "xyz" for by in (1, -1, 2)] + [partner]
    for peer in peers:
        pl.semaphore_signal(barrier, inc=1, device_id=peer, device_id_type=MESH)
    for c in first:
        c.wait()
    pl.semaphore_wait(barrier, len(peers))

    stages = []
    for s in range(2):
        stages.append([
            (land, (s,), pl.ds(0, 384), ORDERS[0]),
            (land, (s,), pl.ds(384, 384), ORDERS[1]),
            (land, (s,), pl.ds(768, 256), ORDERS[2]),
        ])
    stages[0].append((norms, (), EVERY, ORDERS[2]))
    late = [(xs, (0, 0), EVERY, ORDERS[0]), (xs, (0, 1), EVERY, ORDERS[1])]

    def block(part, phase, shift, line=None):
        buf, lead, cols, order = part
        index = [*lead, core]
        for a in "zyx":
            if a == order[phase]:
                index.append(lax.rem(at[a] + shift + 4, 4))
            elif line is not None and a == order[1]:
                index.append(lax.rem(at[a] + line + 4, 4))
            elif a in order[:phase]:
                index.append(EVERY)
            else:
                index.append(at[a])
        return buf.at[tuple(index + [EVERY, cols])]

    sent, forwarded = [], []

    def send(part, phase, shift, by, line=None):
        k = len(sent)
        ref = block(part, phase, shift, line)
        c = pltpu.make_async_remote_copy(
            src_ref=ref, dst_ref=ref, send_sem=send_sem.at[k], recv_sem=recv_sem.at[k],
            device_id=neighbour(core, at, part[3][phase], by), device_id_type=MESH,
        )
        c.start()
        sent.append(c)
        return c

    def forward(part, phase, shift):
        k = len(forwarded)
        ref = block(part, phase, shift)
        c = pltpu.make_async_remote_copy(
            src_ref=ref, dst_ref=ref, send_sem=fsend.at[k], recv_sem=frecv.at[k],
            device_id=partner, device_id_type=MESH,
        )
        c.start()
        forwarded.append(c)
        return c

    def around(parts, phase):
        return {-by: [send(part, phase, 0, by) for part in parts] for by in (2, 1, -1)}

    def receive(copies):
        for c in copies:
            c.wait_recv()

    def receive_ring(copies):
        for by in (1, -1, -2):
            receive(copies[by])

    here, there = stages
    lines_of = ((0, None), (1, 1), (-1, -1), (2, -2))
    handed = [[], []]
    ring = [around(parts, 0) for parts in (stages[0][:3], stages[1])]
    offset = lax.rem(at["y"], 2) * 64 + at["x"] * 16
    spot = lax.broadcasted_iota(jnp.int32, (16, 128), 1) == lax.broadcasted_iota(jnp.int32, (16, 128), 0) + offset
    lines = []
    for s in range(2):
        mine = land[(s, *own)].astype(F32)
        own_sq = jnp.sum(mine * mine, axis=1, keepdims=True) * scale
        lines.append(jnp.sum(jnp.where(spot, own_sq, 0.0), axis=0, keepdims=True))
    norms[own] = jnp.concatenate(lines, axis=0)
    image[...] = jnp.zeros_like(image)
    csum[0] = jnp.zeros(csum.shape[1:], F32)
    for by, copies in around(here[3:], 0).items():
        ring[0][by] += copies
    points_copy.wait()
    wide = points[...].astype(F32)
    factor[...] = jnp.sum(wide * wide, axis=1, keepdims=True) * scale
    here_up, here_down, there_down = [], [], []
    receive_ring(ring[0])
    ring[0] = around(here, 1)
    here_up.append([send(part, 2, 0, 1, 0) for part in here])
    here_down.append([send(part, 2, 0, -1, 0) for part in here])
    receive_ring(ring[1])
    ring[1] = around(there, 1)
    there_down.append([send(part, 2, 0, -1, 0) for part in there])
    for line, source in lines_of[1:]:
        receive(ring[0][source])
        here_up.append([send(part, 2, 0, 1, line) for part in here])
        here_down.append([send(part, 2, 0, -1, line) for part in here])
    handed[0] += [forward(part, 2, 0) for part in here]
    here_far = []

    def relay_up(n):
        receive(here_up[n])
        here_far.append([send(part, 2, -1, 1, lines_of[n][0]) for part in here])

    relay_up(0)
    for line, source in lines_of[1:]:
        receive(ring[1][source])
        there_down.append([send(part, 2, 0, -1, line) for part in there])
    handed[1] += [forward(part, 2, 0) for part in there]
    for n in (1, 2, 3):
        relay_up(n)
    there_up = [send(part, 2, 0, 1) for part in there]
    handed[0] += [forward(part, 2, -1) for part in here]
    for copies in here_down:
        receive(copies)
    handed[0] += [forward(part, 2, 1) for part in here]
    there_far = []
    for n in range(4):
        receive(there_down[n])
        there_far.append([send(part, 2, 1, -1, lines_of[n][0]) for part in there])
    handed[1] += [forward(part, 2, 1) for part in there]
    for copies in here_far:
        receive(copies)
    handed[0] += [forward(part, 2, 2) for part in here]
    late_ring = around(late, 0)

    def own_norms(s):
        wide = land[s, core].reshape(half // 2, 1024).astype(F32)
        rows = pl.ds(s * (half // 2), half // 2)
        col_scale[rows, :] = jnp.sum(wide * wide, axis=1, keepdims=True) * scale

    def norms_line(c):
        for z in range(4):
            for pair in range(2):
                lines = norms[c, z, 2 * pair, 0]
                for a, x in [(0, 1), (0, 2), (0, 3), (1, 0), (1, 1), (1, 2), (1, 3)]:
                    lines += norms[c, z, 2 * pair + a, x]
                q = pl.multiple_of((c * 8 + z * 2 + pair) * 128, 128)
                sq[:, pl.ds(q, 128)] = lines[0:1]
                sq[:, pl.ds(half + q, 128)] = lines[1:2]

    norms_line(core)

    def weights_copy(j, slot):
        return pltpu.make_async_copy(
            upper.at[:, pl.ds(pl.multiple_of(1024 + slot * 512, 512), 512)],
            weights_out.at[:, pl.ds(pl.multiple_of(j * 512, 512), 512)],
            w_sem.at[slot],
        )

    def point_chunk(k, _):
        slot = lax.rem(k, 2)

        @pl.when(k >= 2)
        def _():
            weights_copy(k - 2, slot).wait()

        s, c = k // 4, lax.rem(lax.rem(k // 2, 2) + core, 2)
        j = s * 4 + c * 2 + slot
        rows = land[s, c, pl.ds(slot * 2, 2)].reshape(512, 1024)
        cols = pl.ds(pl.multiple_of(j * 512, 512), 512)
        close = jnp.exp2(dot_nt(points[...], rows) * (2.0 * scale) - (factor[...] + sq[:, cols]))
        upper[:, pl.ds(pl.multiple_of(1024 + slot * 512, 512), 512)] = close.astype(BF16)
        image[:count, 128:] += close[:, :128] + close[:, 128:256] + close[:, 256:384] + close[:, 384:]
        weights_copy(j, slot).start()
        return 0

    lax.fori_loop(0, 2, point_chunk, 0)
    receive(there_up)
    handed[1] += [forward(part, 2, -1) for part in there]
    for copies in there_far:
        receive(copies)
    handed[1] += [forward(part, 2, 2) for part in there]
    receive_ring(late_ring)
    late_ring = around(late, 1)
    receive(handed[0])
    norms_line(1 - core)
    lax.fori_loop(2, 4, point_chunk, 0)
    own_norms(0)
    own_norms(1)
    receive(handed[1])
    lax.fori_loop(4, 8, point_chunk, 0)
    factor[...] = 64.0 / jnp.sqrt(jnp.sum(image[:count, 128:], axis=1, keepdims=True))
    receive_ring(late_ring)
    late_up = [send(part, 2, 0, 1) for part in late]
    late_down = [send(part, 2, 0, -1) for part in late]
    late_handed = [forward(part, 2, 0) for part in late]

    def land_chunk(j, _):
        rows = land[j // 8, lax.rem(j // 4, 2), lax.rem(j, 4)].reshape(256, 1024)
        cols = pl.ds(pl.multiple_of(j * 256, 256), 256)
        inner = dot_nt(land[:, core].reshape(half, 1024), rows)
        close = jnp.exp2(inner * (2.0 * scale) - (col_scale[...] + sq[:, cols]))
        kern[:, cols] = close
        image[:, :128] += close[:, :128] + close[:, 128:]
        csum[0, :, cols] += jnp.sum(close.reshape(half // 8, 8, 256), axis=0)
        return 0

    lax.fori_loop(0, 6, land_chunk, 0)
    receive(late_up + late_down)
    late_far = [send(late[0], 2, -1, 1), send(late[1], 2, 1, -1)]
    late_handed += [forward(part, 2, by) for part in late for by in (-1, 1)]
    lax.fori_loop(6, 12, land_chunk, 0)
    receive(late_far)
    late_handed += [forward(part, 2, 2) for part in late]
    lax.fori_loop(12, 16, land_chunk, 0)

    def swap(src, dst, sems, index):
        c = pltpu.make_async_remote_copy(
            src_ref=src, dst_ref=dst, send_sem=sems.at[0, index], recv_sem=sems.at[1, index],
            device_id=partner, device_id_type=MESH,
        )
        c.start()
        return c

    give = swap(csum.at[0], csum.at[1], c_sem, 0)
    col_scale[...] = 1.0 / jnp.sqrt(jnp.sum(image[:, :128], axis=1, keepdims=True))
    weights_copy(6, 0).wait()
    weights_copy(7, 1).wait()
    receive(late_handed)
    for c in sent + forwarded:
        c.wait_send()
    give.wait_recv()
    row_scale[...] = 1.0 / jnp.sqrt(jnp.sum(csum[0] + csum[1], axis=0, keepdims=True))
    give.wait_send()

    def low_piece(t, s, c):
        return land[s, c, pl.ds(2 * t, 2)].reshape(512, 1024)

    def up_piece(t, s, c):
        cols = pl.ds(pl.multiple_of(s * 2048 + c * 1024, 1024), 1024)
        return upper[pl.ds(pl.multiple_of(t * 512, 512), 512), cols]

    def half_product(piece, t, slot, c):
        rows = jnp.concatenate([piece(t, 0, c), piece(t, 1, c)], axis=1)
        return jnp.dot(rows, xs[slot, :, c].reshape(half, 256), preferred_element_type=F32)

    def scaled(r, b):
        cols = pl.ds(b * 1024, 1024)
        return (kern[r, cols] * col_scale[r, :] * row_scale[:, cols]).astype(BF16)

    def first_low(t, _):
        r = pl.ds(pl.multiple_of(t * 512, 512), 512)
        pieces = []
        for b in range(4):
            piece = scaled(r, b)
            land[b // 2, b % 2, pl.ds(2 * t, 2)] = piece.reshape(2, 4, 4, 16, 1024)
            pieces.append(piece)
        rows = jnp.concatenate(pieces, axis=1)
        image[r, :] = jnp.dot(rows, xs[0].reshape(2 * half, 256), preferred_element_type=F32)
        return 0

    def first_up(t, _):
        r = pl.ds(pl.multiple_of(1024 + t * 512, 512), 512)
        u = pl.ds(pl.multiple_of(t * 512, 512), 512)
        for b in range(4):
            upper[u, pl.ds(b * 1024, 1024)] = scaled(r, b)
        image[r, :] = jnp.dot(upper[u, :], xs[0].reshape(2 * half, 256), preferred_element_type=F32)
        return 0

    eye = lax.broadcasted_iota(jnp.int32, (256, 256), 0) == lax.broadcasted_iota(jnp.int32, (256, 256), 1)
    pending, gives = [], []
    for step in range(ITERS):
        last = step == ITERS - 1
        if step == 0:
            lax.fori_loop(0, 2, first_low, 0)
            lax.fori_loop(0, 2, first_up, 0)
        else:
            def product(piece, base, c, add):
                def tile(t, _):
                    r = pl.ds(pl.multiple_of(base + t * 512, 512), 512)
                    out = half_product(piece, t, step, c)
                    image[r, :] = image[r, :] + out if add else out
                    return 0

                lax.fori_loop(0, 2, tile, 0)

            product(low_piece, 0, core, False)
            product(up_piece, 1024, core, False)
            receive(gives)
            product(up_piece, 1024, 1 - core, True)
            if last:
                weights_in = pltpu.make_async_copy(weights_out, upper, w_sem.at[0])
                weights_in.start()
            product(low_piece, 0, 1 - core, True)
        hi, lo = split(image[...])
        gram = dot_tn(hi, jnp.concatenate([hi, lo], axis=1))
        cross = gram[:, 256:]
        grams[step, 0] = gram[:, :256] + cross + cross.T
        give = swap(grams.at[step, 0], grams.at[step, 1], g_sem, step)
        aug[:, 256:] = jnp.where(eye, 1.0, 0.0)
        give.wait_recv()
        aug[:, :256] = grams[step, 0] + grams[step, 1]
        pending.append(give)
        cholesky_inverse(aug, lower_t, inverse)
        ihi, ilo = split(inverse[...])
        stacked = jnp.concatenate([ihi, ilo, ihi], axis=1)
        if last:
            inverse_lam = 1.0 / jnp.sum(jnp.where(eye, lower_t[...], 0.0), axis=0, keepdims=True)
        gives = []
        target = 0 if last else step + 1
        for t in range(2):
            r = pl.ds(t * 1024, 1024)
            hi, lo = split(image[r, :])
            ortho = dot_nt(jnp.concatenate([hi, hi, lo], axis=1), stacked)
            if last:
                image[r, :] = ortho
                ortho = ortho * col_scale[r, :] * inverse_lam
            xs[target, t, core] = ortho.astype(BF16).reshape(4, 4, 4, 16, 256)
            part = xs.at[target, t, core]
            gives.append(swap(part, part, s_sem if last else x_sem, t))
        pending += gives

    index = at["z"] * 16 + at["y"] * 4 + at["x"]
    for s in range(2):
        rows = pl.ds(pl.multiple_of(s * 1024 + index * 16, 16), 16)
        own_out[16 * s : 16 * s + 16, :] = image[rows, :]
    weights_in.wait()
    for t in range(2):
        image[t * 512 : t * 512 + 512, :] = half_product(up_piece, t, 0, core)
    receive(gives)
    copies = []
    for t in range(2):
        r = pl.ds(t * 512, 512)
        image[r, :] = (image[r, :] + half_product(up_piece, t, 0, 1 - core)) * factor[r, :]
        copies.append(pltpu.make_async_copy(image.at[r, :], coords_out.at[r, :], o_sem.at[t]))
        copies[-1].start()
    for c in pending:
        c.wait_send()
    for c in copies:
        c.wait()


def deliver_kernel(own_ref, coords_ref, own_out, coords_out):
    own_out[...] = own_ref[...]
    coords_out[...] = coords_ref[...]


def body(landmarks, initial_basis, points):
    shard, width = landmarks.shape
    rank = initial_basis.shape[1]
    total = shard * 128
    half = total // 2
    count = points.shape[0]
    scale = LOG2E / (SPREAD * width)
    anywhere = pl.BlockSpec(memory_space=pl.ANY)
    vmem = pl.BlockSpec(memory_space=pltpu.VMEM)
    dma = pltpu.SemaphoreType.DMA
    results = (jax.ShapeDtypeStruct((shard, rank), F32), jax.ShapeDtypeStruct((count, rank), F32))

    own, coords, _ = pl.pallas_call(
        functools.partial(nystrom_kernel, scale),
        name="nystrom",
        out_shape=(*results, jax.ShapeDtypeStruct((count, total), BF16)),
        in_specs=[anywhere, anywhere, anywhere],
        out_specs=(vmem, anywhere, anywhere),
        scratch_shapes=[
            pltpu.VMEM((2, 2, 4, 4, 4, shard // 2, width), BF16),
            pltpu.VMEM((2, 2, 2, 4, 4, 4, shard // 2, rank), BF16),
            pltpu.VMEM((2, 4, 4, 4, 2, 128), F32),
            pltpu.VMEM((half, total), F32),
            pltpu.VMEM((count, total), BF16),
            pltpu.VMEM((half, rank), F32),
            pltpu.VMEM((1, total), F32),
            pltpu.VMEM((2, 8, total), F32),
            pltpu.VMEM((2, 2, rank, rank), F32),
            pltpu.VMEM((rank, 2 * rank), F32),
            pltpu.VMEM((rank, rank), F32),
            pltpu.VMEM((rank, rank), F32),
            pltpu.VMEM((half, 1), F32),
            pltpu.VMEM((1, total), F32),
            pltpu.VMEM((count, 1), F32),
            dma((5,)), dma((135,)), dma((135,)), dma((36,)), dma((36,)), dma((2,)),
            dma((2, 1)), dma((2, 2)), dma((2, 2)), dma((2, 2)), dma((2,)),
        ],
        compiler_params=pltpu.CompilerParams(
            collective_id=0, has_side_effects=True, vmem_limit_bytes=VMEM_LIMIT
        ),
    )(landmarks, initial_basis, points)
    return pl.pallas_call(
        deliver_kernel,
        name="deliver",
        out_shape=results,
        in_specs=[vmem, vmem],
        out_specs=(vmem, vmem),
    )(own, coords)


def solution(mesh):
    in_specs = (P(("grp", "row"), None), P(("grp", "row"), None), P(("grp", "row"), None))
    out_specs = (P(("grp", "row"), None), P(("grp", "row"), None))
    return jax.shard_map(body, mesh=mesh, in_specs=in_specs, out_specs=out_specs, check_vma=False)
```

```python
import functools
import math

import jax
import jax.numpy as jnp
from jax import lax
from jax.experimental import pallas as pl
from jax.experimental.pallas import tpu as pltpu
from jax.sharding import PartitionSpec as P

ITERS = 2
SPREAD = 0.25
LOG2E = 1.4426950408889634
MESH = pl.DeviceIdType.MESH
F32 = jnp.float32
BF16 = jnp.bfloat16
VMEM_LIMIT = 67_043_328


def place():
    grp, row = lax.axis_index("grp"), lax.axis_index("row")
    core, y_hi = lax.rem(grp, 2), grp // 2
    y_lo, z, x = row // 16, lax.rem(row // 4, 4), lax.rem(row, 4)
    return core, {"z": z, "y": y_hi * 2 + y_lo, "x": x}


def device(core, at):
    return ((at["y"] // 2) * 2 + core, lax.rem(at["y"], 2) * 16 + at["z"] * 4 + at["x"])


def neighbour(core, at, axis, by):
    return device(core, {**at, axis: lax.rem(at[axis] + by + 4, 4)})


def dot_nt(a, b):
    return lax.dot_general(a, b, (((1,), (1,)), ((), ())), preferred_element_type=F32)


def dot_tn(a, b):
    return lax.dot_general(a, b, (((0,), (0,)), ((), ())), preferred_element_type=F32)


ORDERS = (("x", "y", "z"), ("y", "z", "x"), ("z", "x", "y"))
EVERY = slice(None)


def split(x):
    hi = x.astype(BF16)
    return hi, (x - hi.astype(F32)).astype(BF16)


def in_three(x):
    hi = x.astype(BF16)
    rest = x - hi.astype(F32)
    mid = rest.astype(BF16)
    return hi, mid, (rest - mid.astype(F32)).astype(BF16)


def cholesky_inverse(aug, lower_t, inverse):
    lane, size = 128, 32
    row_id = lax.broadcasted_iota(jnp.int32, (size, lane), 0)
    for r0 in range(0, 256, size):
        end = r0 + size
        diag = aug[pl.ds(r0, size), :256]
        reps = [jnp.broadcast_to(diag[:, r0 + j : r0 + j + 1], (size, lane)) for j in range(size)]
        panel = [aug[pl.ds(r0, size), pl.ds(k * lane, lane)] for k in range(4)]
        live = [k for k in range(4) if (k < 2 and (k + 1) * lane > r0) or (k >= 2 and (k - 2) * lane < end)]
        for j in range(size):
            root = lax.rsqrt(reps[j][j : j + 1, :])
            column = reps[j] * root
            for i in range(j + 1, size):
                reps[i] = reps[i] - column * column[i : i + 1, :]
            below = jnp.where(row_id > j, column, 0.0)
            for k in live:
                line = panel[k][j : j + 1, :] * root
                panel[k] = jnp.where(row_id == j, line, panel[k] - below * line)
        for k in range(2):
            lower_t[pl.ds(r0, size), pl.ds(k * lane, lane)] = panel[k]
            inverse[pl.ds(r0, size), pl.ds(k * lane, lane)] = panel[2 + k]
        if end < 256:
            start = end // lane * lane
            after = [k for k in range(4) if (k < 2 and k * lane >= start) or (k >= 2 and (k - 2) * lane < end)]
            terms = [in_three(panel[k]) for k in range(4)]

            def stack(columns, order):
                return jnp.concatenate(
                    [jnp.concatenate([terms[k][o] for o in order], axis=0) for k in columns], axis=1
                )

            left = stack(range(start // lane, 2), (0, 0, 1, 1, 0, 2))
            change = dot_tn(left, stack(after, (0, 1, 0, 1, 2, 0)))
            for n, k in enumerate(after):
                cols = pl.ds(k * lane, lane)
                aug[start:, cols] = aug[start:, cols] - change[:, n * lane : (n + 1) * lane]


def nystrom_kernel(
    scale, land_in, basis_in, points_in,
    own_out, coords_out, weights_out,
    land, xs, norms, kern, upper, image, sq, csum, grams, aug, lower_t, inverse,
    col_scale, row_scale, factor,
    own_sem, send_sem, recv_sem, fsend, frecv, w_sem, c_sem, g_sem, x_sem, s_sem, o_sem,
):
    core, at = place()
    partner = device(1 - core, at)
    own = (core, at["z"], at["y"], at["x"])
    half = kern.shape[0]
    count = points_in.shape[0]

    first = []
    for s in range(2):
        rows = pl.ds(16 * s, 16)
        first.append(pltpu.make_async_copy(land_in.at[rows, :], land.at[(s, *own)], own_sem.at[s]))
        first.append(pltpu.make_async_copy(basis_in.at[rows, :], xs.at[(0, s, *own)], own_sem.at[2 + s]))
    for c in first:
        c.start()
    points = upper.at[:, pl.ds(0, 1024)]
    points_copy = pltpu.make_async_copy(points_in, points, own_sem.at[4])
    points_copy.start()
    barrier = pltpu.get_barrier_semaphore()
    peers = [neighbour(core, at, a, by) for a in "xyz" for by in (1, -1, 2)] + [partner]
    for peer in peers:
        pl.semaphore_signal(barrier, inc=1, device_id=peer, device_id_type=MESH)
    for c in first:
        c.wait()
    pl.semaphore_wait(barrier, len(peers))

    stages = []
    for s in range(2):
        stages.append([
            (land, (s,), pl.ds(0, 384), ORDERS[0]),
            (land, (s,), pl.ds(384, 384), ORDERS[1]),
            (land, (s,), pl.ds(768, 256), ORDERS[2]),
        ])
    stages[0].append((norms, (), EVERY, ORDERS[2]))
    late = [(xs, (0, 0), EVERY, ORDERS[0]), (xs, (0, 1), EVERY, ORDERS[1])]

    def block(part, phase, shift, line=None):
        buf, lead, cols, order = part
        index = [*lead, core]
        for a in "zyx":
            if a == order[phase]:
                index.append(lax.rem(at[a] + shift + 4, 4))
            elif line is not None and a == order[1]:
                index.append(lax.rem(at[a] + line + 4, 4))
            elif a in order[:phase]:
                index.append(EVERY)
            else:
                index.append(at[a])
        return buf.at[tuple(index + [EVERY, cols])]

    sent, forwarded = [], []

    def send(part, phase, shift, by, line=None):
        k = len(sent)
        ref = block(part, phase, shift, line)
        c = pltpu.make_async_remote_copy(
            src_ref=ref, dst_ref=ref, send_sem=send_sem.at[k], recv_sem=recv_sem.at[k],
            device_id=neighbour(core, at, part[3][phase], by), device_id_type=MESH,
        )
        c.start()
        sent.append(c)
        return c

    def forward(part, phase, shift):
        k = len(forwarded)
        ref = block(part, phase, shift)
        c = pltpu.make_async_remote_copy(
            src_ref=ref, dst_ref=ref, send_sem=fsend.at[k], recv_sem=frecv.at[k],
            device_id=partner, device_id_type=MESH,
        )
        c.start()
        forwarded.append(c)
        return c

    def around(parts, phase):
        return {-by: [send(part, phase, 0, by) for part in parts] for by in (2, 1, -1)}

    def receive(copies):
        for c in copies:
            c.wait_recv()

    def receive_ring(copies):
        for by in (1, -1, -2):
            receive(copies[by])

    here, there = stages
    lines_of = ((0, None), (1, 1), (-1, -1), (2, -2))
    handed = [[], []]
    ring = [around(parts, 0) for parts in (stages[0][:3], stages[1])]
    offset = lax.rem(at["y"], 2) * 64 + at["x"] * 16
    spot = lax.broadcasted_iota(jnp.int32, (16, 128), 1) == lax.broadcasted_iota(jnp.int32, (16, 128), 0) + offset
    lines = []
    for s in range(2):
        mine = land[(s, *own)].astype(F32)
        own_sq = jnp.sum(mine * mine, axis=1, keepdims=True) * scale
        lines.append(jnp.sum(jnp.where(spot, own_sq, 0.0), axis=0, keepdims=True))
    norms[own] = jnp.concatenate(lines, axis=0)
    image[...] = jnp.zeros_like(image)
    csum[0] = jnp.zeros(csum.shape[1:], F32)
    for by, copies in around(here[3:], 0).items():
        ring[0][by] += copies
    points_copy.wait()
    wide = points[...].astype(F32)
    factor[...] = jnp.sum(wide * wide, axis=1, keepdims=True) * scale
    here_up, here_down, there_down = [], [], []
    receive_ring(ring[0])
    ring[0] = around(here, 1)
    here_up.append([send(part, 2, 0, 1, 0) for part in here])
    here_down.append([send(part, 2, 0, -1, 0) for part in here])
    receive_ring(ring[1])
    ring[1] = around(there, 1)
    there_down.append([send(part, 2, 0, -1, 0) for part in there])
    for line, source in lines_of[1:]:
        receive(ring[0][source])
        here_up.append([send(part, 2, 0, 1, line) for part in here])
        here_down.append([send(part, 2, 0, -1, line) for part in here])
    handed[0] += [forward(part, 2, 0) for part in here]
    here_far = []

    def relay_up(n):
        receive(here_up[n])
        here_far.append([send(part, 2, -1, 1, lines_of[n][0]) for part in here])

    relay_up(0)
    for line, source in lines_of[1:]:
        receive(ring[1][source])
        there_down.append([send(part, 2, 0, -1, line) for part in there])
    handed[1] += [forward(part, 2, 0) for part in there]
    for n in (1, 2, 3):
        relay_up(n)
    there_up = [send(part, 2, 0, 1) for part in there]
    handed[0] += [forward(part, 2, -1) for part in here]
    for copies in here_down:
        receive(copies)
    handed[0] += [forward(part, 2, 1) for part in here]
    there_far = []
    for n in range(4):
        receive(there_down[n])
        there_far.append([send(part, 2, 1, -1, lines_of[n][0]) for part in there])
    handed[1] += [forward(part, 2, 1) for part in there]
    for copies in here_far:
        receive(copies)
    handed[0] += [forward(part, 2, 2) for part in here]
    late_ring = around(late, 0)

    def norms_line(c):
        for z in range(4):
            for pair in range(2):
                lines = norms[c, z, 2 * pair, 0]
                for a, x in [(0, 1), (0, 2), (0, 3), (1, 0), (1, 1), (1, 2), (1, 3)]:
                    lines += norms[c, z, 2 * pair + a, x]
                q = pl.multiple_of((c * 8 + z * 2 + pair) * 128, 128)
                sq[:, pl.ds(q, 128)] = lines[0:1]
                sq[:, pl.ds(half + q, 128)] = lines[1:2]

    norms_line(core)

    def weights_copy(j, slot):
        return pltpu.make_async_copy(
            upper.at[:, pl.ds(pl.multiple_of(1024 + slot * 512, 512), 512)],
            weights_out.at[:, pl.ds(pl.multiple_of(j * 512, 512), 512)],
            w_sem.at[slot],
        )

    def point_chunk(k, _):
        slot = lax.rem(k, 2)

        @pl.when(k >= 2)
        def _():
            weights_copy(k - 2, slot).wait()

        s, c = k // 4, lax.rem(lax.rem(k // 2, 2) + core, 2)
        j = s * 4 + c * 2 + slot
        rows = land[s, c, pl.ds(slot * 2, 2)].reshape(512, 1024)
        cols = pl.ds(pl.multiple_of(j * 512, 512), 512)
        close = jnp.exp2(dot_nt(points[...], rows) * (2.0 * scale) - (factor[...] + sq[:, cols]))
        upper[:, pl.ds(pl.multiple_of(1024 + slot * 512, 512), 512)] = close.astype(BF16)
        image[:count, 128:] += close[:, :128] + close[:, 128:256] + close[:, 256:384] + close[:, 384:]
        weights_copy(j, slot).start()
        return 0

    def early_chunk(k, _):
        wide = land[k // 2, core, pl.ds(lax.rem(k, 2) * 2, 2)].reshape(512, 1024).astype(F32)
        rows = pl.ds(pl.multiple_of(k * 512, 512), 512)
        col_scale[rows, :] = jnp.sum(wide * wide, axis=1, keepdims=True) * scale
        return point_chunk(k, 0)

    lax.fori_loop(0, 2, early_chunk, 0)
    receive(there_up)
    handed[1] += [forward(part, 2, -1) for part in there]
    for copies in there_far:
        receive(copies)
    handed[1] += [forward(part, 2, 2) for part in there]
    receive_ring(late_ring)
    late_ring = around(late, 1)
    receive(handed[0])
    norms_line(1 - core)
    lax.fori_loop(2, 4, early_chunk, 0)
    receive(handed[1])
    lax.fori_loop(4, 8, point_chunk, 0)
    factor[...] = 64.0 / jnp.sqrt(jnp.sum(image[:count, 128:], axis=1, keepdims=True))
    receive_ring(late_ring)
    late_up = [send(part, 2, 0, 1) for part in late]
    late_down = [send(part, 2, 0, -1) for part in late]
    late_handed = [forward(part, 2, 0) for part in late]

    def land_chunk(j, _):
        rows = land[j // 8, lax.rem(j // 4, 2), lax.rem(j, 4)].reshape(256, 1024)
        cols = pl.ds(pl.multiple_of(j * 256, 256), 256)
        inner = dot_nt(land[:, core].reshape(half, 1024), rows)
        close = jnp.exp2(inner * (2.0 * scale) - (col_scale[...] + sq[:, cols]))
        kern[:, cols] = close
        image[:, :128] += close[:, :128] + close[:, 128:]
        csum[0, :, cols] += jnp.sum(close.reshape(half // 8, 8, 256), axis=0)
        return 0

    lax.fori_loop(0, 8, land_chunk, 0)
    receive(late_up + late_down)
    late_far = [send(late[0], 2, -1, 1), send(late[1], 2, 1, -1)]
    late_handed += [forward(part, 2, by) for part in late for by in (-1, 1)]
    lax.fori_loop(8, 16, land_chunk, 0)
    receive(late_far)
    late_handed += [forward(part, 2, 2) for part in late]

    def swap(src, dst, sems, index):
        c = pltpu.make_async_remote_copy(
            src_ref=src, dst_ref=dst, send_sem=sems.at[0, index], recv_sem=sems.at[1, index],
            device_id=partner, device_id_type=MESH,
        )
        c.start()
        return c

    give = swap(csum.at[0], csum.at[1], c_sem, 0)
    col_scale[...] = 1.0 / jnp.sqrt(jnp.sum(image[:, :128], axis=1, keepdims=True))
    weights_copy(6, 0).wait()
    weights_copy(7, 1).wait()
    receive(late_handed)
    for c in sent + forwarded:
        c.wait_send()
    give.wait_recv()
    row_scale[...] = 1.0 / jnp.sqrt(jnp.sum(csum[0] + csum[1], axis=0, keepdims=True))
    give.wait_send()

    def low_piece(s, c):
        return land[s, c].reshape(1024, 1024)

    def up_piece(s, c):
        return upper[:, pl.ds(pl.multiple_of(s * 2048 + c * 1024, 1024), 1024)]

    def half_product(piece, slot, c):
        rows = jnp.concatenate([piece(0, c), piece(1, c)], axis=1)
        return jnp.dot(rows, xs[slot, :, c].reshape(half, 256), preferred_element_type=F32)

    def scaled(r, b):
        cols = pl.ds(b * 1024, 1024)
        return (kern[r, cols] * col_scale[r, :] * row_scale[:, cols]).astype(BF16)

    def first_low(t, _):
        r = pl.ds(pl.multiple_of(t * 512, 512), 512)
        pieces = []
        for b in range(4):
            piece = scaled(r, b)
            land[b // 2, b % 2, pl.ds(2 * t, 2)] = piece.reshape(2, 4, 4, 16, 1024)
            pieces.append(piece)
        rows = jnp.concatenate(pieces, axis=1)
        image[r, :] = jnp.dot(rows, xs[0].reshape(2 * half, 256), preferred_element_type=F32)
        return 0

    def first_up(t, _):
        r = pl.ds(pl.multiple_of(1024 + t * 512, 512), 512)
        u = pl.ds(pl.multiple_of(t * 512, 512), 512)
        for b in range(4):
            upper[u, pl.ds(b * 1024, 1024)] = scaled(r, b)
        image[r, :] = jnp.dot(upper[u, :], xs[0].reshape(2 * half, 256), preferred_element_type=F32)
        return 0

    eye = lax.broadcasted_iota(jnp.int32, (256, 256), 0) == lax.broadcasted_iota(jnp.int32, (256, 256), 1)
    pending, gives = [], []
    for step in range(ITERS):
        last = step == ITERS - 1
        if step == 0:
            lax.fori_loop(0, 2, first_low, 0)
            lax.fori_loop(0, 2, first_up, 0)
        else:
            def product(piece, base, c, add):
                r = pl.ds(base, 1024)
                out = half_product(piece, step, c)
                image[r, :] = image[r, :] + out if add else out

            product(low_piece, 0, core, False)
            product(up_piece, 1024, core, False)
            receive(gives)
            product(up_piece, 1024, 1 - core, True)
            if last:
                weights_in = pltpu.make_async_copy(weights_out, upper, w_sem.at[0])
                weights_in.start()
            product(low_piece, 0, 1 - core, True)
        hi, lo = split(image[...])
        gram = dot_tn(hi, jnp.concatenate([hi, lo], axis=1))
        cross = gram[:, 256:]
        grams[step, 0] = gram[:, :256] + cross + cross.T
        give = swap(grams.at[step, 0], grams.at[step, 1], g_sem, step)
        aug[:, 256:] = jnp.where(eye, 1.0, 0.0)
        give.wait_recv()
        aug[:, :256] = grams[step, 0] + grams[step, 1]
        pending.append(give)
        cholesky_inverse(aug, lower_t, inverse)
        ihi, ilo = split(inverse[...])
        stacked = jnp.concatenate([ihi, ilo, ihi], axis=1)
        if last:
            inverse_lam = 1.0 / jnp.sum(jnp.where(eye, lower_t[...], 0.0), axis=0, keepdims=True)
        gives = []
        target = 0 if last else step + 1
        for t in range(2):
            r = pl.ds(t * 1024, 1024)
            hi, lo = split(image[r, :])
            ortho = dot_nt(jnp.concatenate([hi, hi, lo], axis=1), stacked)
            if last:
                image[r, :] = ortho
                ortho = ortho * col_scale[r, :] * inverse_lam
            xs[target, t, core] = ortho.astype(BF16).reshape(4, 4, 4, 16, 256)
            part = xs.at[target, t, core]
            gives.append(swap(part, part, s_sem if last else x_sem, t))
        pending += gives

    index = at["z"] * 16 + at["y"] * 4 + at["x"]
    for s in range(2):
        rows = pl.ds(pl.multiple_of(s * 1024 + index * 16, 16), 16)
        own_out[16 * s : 16 * s + 16, :] = image[rows, :]
    weights_in.wait()
    image[:count, :] = half_product(up_piece, 0, core)
    receive(gives)
    r = pl.ds(0, count)
    image[r, :] = (image[r, :] + half_product(up_piece, 0, 1 - core)) * factor[r, :]
    copies = [pltpu.make_async_copy(image.at[r, :], coords_out, o_sem.at[0])]
    copies[0].start()
    for c in pending:
        c.wait_send()
    for c in copies:
        c.wait()


def deliver_kernel(own_ref, coords_ref, own_out, coords_out):
    own_out[...] = own_ref[...]
    coords_out[...] = coords_ref[...]


def body(landmarks, initial_basis, points):
    shard, width = landmarks.shape
    rank = initial_basis.shape[1]
    total = shard * 128
    half = total // 2
    count = points.shape[0]
    scale = LOG2E / (SPREAD * width)
    anywhere = pl.BlockSpec(memory_space=pl.ANY)
    vmem = pl.BlockSpec(memory_space=pltpu.VMEM)
    dma = pltpu.SemaphoreType.DMA
    results = (jax.ShapeDtypeStruct((shard, rank), F32), jax.ShapeDtypeStruct((count, rank), F32))

    own, coords, _ = pl.pallas_call(
        functools.partial(nystrom_kernel, scale),
        name="nystrom",
        out_shape=(*results, jax.ShapeDtypeStruct((count, total), BF16)),
        in_specs=[anywhere, anywhere, anywhere],
        out_specs=(vmem, anywhere, anywhere),
        scratch_shapes=[
            pltpu.VMEM((2, 2, 4, 4, 4, shard // 2, width), BF16),
            pltpu.VMEM((2, 2, 2, 4, 4, 4, shard // 2, rank), BF16),
            pltpu.VMEM((2, 4, 4, 4, 2, 128), F32),
            pltpu.VMEM((half, total), F32),
            pltpu.VMEM((count, total), BF16),
            pltpu.VMEM((half, rank), F32),
            pltpu.VMEM((1, total), F32),
            pltpu.VMEM((2, 8, total), F32),
            pltpu.VMEM((2, 2, rank, rank), F32),
            pltpu.VMEM((rank, 2 * rank), F32),
            pltpu.VMEM((rank, rank), F32),
            pltpu.VMEM((rank, rank), F32),
            pltpu.VMEM((half, 1), F32),
            pltpu.VMEM((1, total), F32),
            pltpu.VMEM((count, 1), F32),
            dma((5,)), dma((135,)), dma((135,)), dma((36,)), dma((36,)), dma((2,)),
            dma((2, 1)), dma((2, 2)), dma((2, 2)), dma((2, 2)), dma((2,)),
        ],
        compiler_params=pltpu.CompilerParams(
            collective_id=0, has_side_effects=True, vmem_limit_bytes=VMEM_LIMIT
        ),
    )(landmarks, initial_basis, points)
    return pl.pallas_call(
        deliver_kernel,
        name="deliver",
        out_shape=results,
        in_specs=[vmem, vmem],
        out_specs=(vmem, vmem),
    )(own, coords)


def solution(mesh):
    in_specs = (P(("grp", "row"), None), P(("grp", "row"), None), P(("grp", "row"), None))
    out_specs = (P(("grp", "row"), None), P(("grp", "row"), None))
    return jax.shard_map(body, mesh=mesh, in_specs=in_specs, out_specs=out_specs, check_vma=False)
```

```python
import functools
import math

import jax
import jax.numpy as jnp
from jax import lax
from jax.experimental import pallas as pl
from jax.experimental.pallas import tpu as pltpu
from jax.sharding import PartitionSpec as P

ITERS = 2
SPREAD = 0.25
LOG2E = 1.4426950408889634
MESH = pl.DeviceIdType.MESH
F32 = jnp.float32
BF16 = jnp.bfloat16
VMEM_LIMIT = 67_043_328


def place():
    grp, row = lax.axis_index("grp"), lax.axis_index("row")
    core, y_hi = lax.rem(grp, 2), grp // 2
    y_lo, z, x = row // 16, lax.rem(row // 4, 4), lax.rem(row, 4)
    return core, {"z": z, "y": y_hi * 2 + y_lo, "x": x}


def device(core, at):
    return ((at["y"] // 2) * 2 + core, lax.rem(at["y"], 2) * 16 + at["z"] * 4 + at["x"])


def neighbour(core, at, axis, by):
    return device(core, {**at, axis: lax.rem(at[axis] + by + 4, 4)})


def dot_nt(a, b):
    return lax.dot_general(a, b, (((1,), (1,)), ((), ())), preferred_element_type=F32)


def dot_tn(a, b):
    return lax.dot_general(a, b, (((0,), (0,)), ((), ())), preferred_element_type=F32)


ORDERS = (("x", "y", "z"), ("y", "z", "x"), ("z", "x", "y"))
EVERY = slice(None)


def split(x):
    hi = x.astype(BF16)
    return hi, (x - hi.astype(F32)).astype(BF16)


def in_three(x):
    hi = x.astype(BF16)
    rest = x - hi.astype(F32)
    mid = rest.astype(BF16)
    return hi, mid, (rest - mid.astype(F32)).astype(BF16)


def cholesky_inverse(aug, lower_t, inverse):
    lane, size = 128, 32
    row_id = lax.broadcasted_iota(jnp.int32, (size, lane), 0)
    for r0 in range(0, 256, size):
        end = r0 + size
        diag = aug[pl.ds(r0, size), :256]
        reps = [jnp.broadcast_to(diag[:, r0 + j : r0 + j + 1], (size, lane)) for j in range(size)]
        panel = [aug[pl.ds(r0, size), pl.ds(k * lane, lane)] for k in range(4)]
        live = [k for k in range(4) if (k < 2 and (k + 1) * lane > r0) or (k >= 2 and (k - 2) * lane < end)]
        for j in range(size):
            root = lax.rsqrt(reps[j][j : j + 1, :])
            column = reps[j] * root
            for i in range(j + 1, size):
                reps[i] = reps[i] - column * column[i : i + 1, :]
            below = jnp.where(row_id > j, column, 0.0)
            for k in live:
                line = panel[k][j : j + 1, :] * root
                panel[k] = jnp.where(row_id == j, line, panel[k] - below * line)
        for k in range(2):
            lower_t[pl.ds(r0, size), pl.ds(k * lane, lane)] = panel[k]
            inverse[pl.ds(r0, size), pl.ds(k * lane, lane)] = panel[2 + k]
        if end < 256:
            start = end // lane * lane
            after = [k for k in range(4) if (k < 2 and k * lane >= start) or (k >= 2 and (k - 2) * lane < end)]
            terms = [in_three(panel[k]) for k in range(4)]

            def stack(columns, order):
                return jnp.concatenate(
                    [jnp.concatenate([terms[k][o] for o in order], axis=0) for k in columns], axis=1
                )

            left = stack(range(start // lane, 2), (0, 0, 1, 1, 0, 2))
            change = dot_tn(left, stack(after, (0, 1, 0, 1, 2, 0)))
            for n, k in enumerate(after):
                cols = pl.ds(k * lane, lane)
                aug[start:, cols] = aug[start:, cols] - change[:, n * lane : (n + 1) * lane]


def nystrom_kernel(
    scale, land_in, basis_in, points_in,
    own_out, coords_out, weights_out,
    land, xs, norms, kern, upper, image, sq, csum, grams, aug, lower_t, inverse,
    col_scale, row_scale, factor,
    own_sem, send_sem, recv_sem, fsend, frecv, w_sem, c_sem, g_sem, x_sem, s_sem, o_sem,
):
    core, at = place()
    partner = device(1 - core, at)
    own = (core, at["z"], at["y"], at["x"])
    half = kern.shape[0]
    count = points_in.shape[0]

    first = []
    for s in range(2):
        rows = pl.ds(16 * s, 16)
        first.append(pltpu.make_async_copy(land_in.at[rows, :], land.at[(s, *own)], own_sem.at[s]))
        first.append(pltpu.make_async_copy(basis_in.at[rows, :], xs.at[(0, s, *own)], own_sem.at[2 + s]))
    for c in first:
        c.start()
    points = upper.at[:, pl.ds(0, 1024)]
    points_copy = pltpu.make_async_copy(points_in, points, own_sem.at[4])
    points_copy.start()
    barrier = pltpu.get_barrier_semaphore()
    peers = [neighbour(core, at, a, by) for a in "xyz" for by in (1, -1, 2)] + [partner]
    for peer in peers:
        pl.semaphore_signal(barrier, inc=1, device_id=peer, device_id_type=MESH)
    for c in first:
        c.wait()
    pl.semaphore_wait(barrier, len(peers))

    stages = []
    for s in range(2):
        stages.append([
            (land, (s,), pl.ds(0, 384), ORDERS[0]),
            (land, (s,), pl.ds(384, 384), ORDERS[1]),
            (land, (s,), pl.ds(768, 256), ORDERS[2]),
        ])
    stages[0].append((norms, (), EVERY, ORDERS[2]))
    late = [(xs, (0, 0), EVERY, ORDERS[0]), (xs, (0, 1), EVERY, ORDERS[1])]

    def block(part, phase, shift, line=None):
        buf, lead, cols, order = part
        index = [*lead, core]
        for a in "zyx":
            if a == order[phase]:
                index.append(lax.rem(at[a] + shift + 4, 4))
            elif line is not None and a == order[1]:
                index.append(lax.rem(at[a] + line + 4, 4))
            elif a in order[:phase]:
                index.append(EVERY)
            else:
                index.append(at[a])
        return buf.at[tuple(index + [EVERY, cols])]

    sent, forwarded = [], []

    def send(part, phase, shift, by, line=None):
        k = len(sent)
        ref = block(part, phase, shift, line)
        c = pltpu.make_async_remote_copy(
            src_ref=ref, dst_ref=ref, send_sem=send_sem.at[k], recv_sem=recv_sem.at[k],
            device_id=neighbour(core, at, part[3][phase], by), device_id_type=MESH,
        )
        c.start()
        sent.append(c)
        return c

    def forward(part, phase, shift):
        k = len(forwarded)
        ref = block(part, phase, shift)
        c = pltpu.make_async_remote_copy(
            src_ref=ref, dst_ref=ref, send_sem=fsend.at[k], recv_sem=frecv.at[k],
            device_id=partner, device_id_type=MESH,
        )
        c.start()
        forwarded.append(c)
        return c

    def around(parts, phase):
        return {-by: [send(part, phase, 0, by) for part in parts] for by in (2, 1, -1)}

    def receive(copies):
        for c in copies:
            c.wait_recv()

    def receive_ring(copies):
        for by in (1, -1, -2):
            receive(copies[by])

    here, there = stages
    lines_of = ((0, None), (1, 1), (-1, -1), (2, -2))
    handed = [[], []]
    ring = [around(parts, 0) for parts in (stages[0][:3], stages[1])]
    offset = lax.rem(at["y"], 2) * 64 + at["x"] * 16
    spot = lax.broadcasted_iota(jnp.int32, (16, 128), 1) == lax.broadcasted_iota(jnp.int32, (16, 128), 0) + offset
    lines = []
    for s in range(2):
        mine = land[(s, *own)].astype(F32)
        own_sq = jnp.sum(mine * mine, axis=1, keepdims=True) * scale
        lines.append(jnp.sum(jnp.where(spot, own_sq, 0.0), axis=0, keepdims=True))
    norms[own] = jnp.concatenate(lines, axis=0)
    image[...] = jnp.zeros_like(image)
    csum[0] = jnp.zeros(csum.shape[1:], F32)
    for by, copies in around(here[3:], 0).items():
        ring[0][by] += copies
    points_copy.wait()
    wide = points[...].astype(F32)
    factor[...] = jnp.sum(wide * wide, axis=1, keepdims=True) * scale
    here_up, here_down, there_down = [], [], []
    receive_ring(ring[0])
    ring[0] = around(here, 1)
    here_up.append([send(part, 2, 0, 1, 0) for part in here])
    here_down.append([send(part, 2, 0, -1, 0) for part in here])
    receive_ring(ring[1])
    ring[1] = around(there, 1)
    there_down.append([send(part, 2, 0, -1, 0) for part in there])
    for line, source in lines_of[1:]:
        receive(ring[0][source])
        here_up.append([send(part, 2, 0, 1, line) for part in here])
        here_down.append([send(part, 2, 0, -1, line) for part in here])
    handed[0] += [forward(part, 2, 0) for part in here]
    here_far = []

    def relay_up(n):
        receive(here_up[n])
        here_far.append([send(part, 2, -1, 1, lines_of[n][0]) for part in here])

    relay_up(0)
    for line, source in lines_of[1:]:
        receive(ring[1][source])
        there_down.append([send(part, 2, 0, -1, line) for part in there])
    handed[1] += [forward(part, 2, 0) for part in there]
    for n in (1, 2, 3):
        relay_up(n)
    there_up = [send(part, 2, 0, 1) for part in there]
    handed[0] += [forward(part, 2, -1) for part in here]
    for copies in here_down:
        receive(copies)
    handed[0] += [forward(part, 2, 1) for part in here]
    there_far = []
    for n in range(4):
        receive(there_down[n])
        there_far.append([send(part, 2, 1, -1, lines_of[n][0]) for part in there])
    handed[1] += [forward(part, 2, 1) for part in there]
    for copies in here_far:
        receive(copies)
    handed[0] += [forward(part, 2, 2) for part in here]
    late_ring = around(late, 0)

    def norms_line(c):
        for z in range(4):
            for pair in range(2):
                lines = norms[c, z, 2 * pair, 0]
                for a, x in [(0, 1), (0, 2), (0, 3), (1, 0), (1, 1), (1, 2), (1, 3)]:
                    lines += norms[c, z, 2 * pair + a, x]
                q = pl.multiple_of((c * 8 + z * 2 + pair) * 128, 128)
                sq[:, pl.ds(q, 128)] = lines[0:1]
                sq[:, pl.ds(half + q, 128)] = lines[1:2]

    norms_line(core)

    def weights_copy(j, slot):
        return pltpu.make_async_copy(
            upper.at[:, pl.ds(pl.multiple_of(1024 + slot * 512, 512), 512)],
            weights_out.at[:, pl.ds(pl.multiple_of(j * 512, 512), 512)],
            w_sem.at[slot],
        )

    def point_chunk(k, _):
        slot = lax.rem(k, 2)

        @pl.when(k >= 2)
        def _():
            weights_copy(k - 2, slot).wait()

        s, c = k // 4, lax.rem(lax.rem(k // 2, 2) + core, 2)
        j = s * 4 + c * 2 + slot
        rows = land[s, c, pl.ds(slot * 2, 2)].reshape(512, 1024)
        cols = pl.ds(pl.multiple_of(j * 512, 512), 512)
        close = jnp.exp2(dot_nt(points[...], rows) * (2.0 * scale) - (factor[...] + sq[:, cols]))
        upper[:, pl.ds(pl.multiple_of(1024 + slot * 512, 512), 512)] = close.astype(BF16)
        image[:count, 128:] += close[:, :128] + close[:, 128:256] + close[:, 256:384] + close[:, 384:]
        weights_copy(j, slot).start()
        return 0

    def early_chunk(k, _):
        wide = land[k // 2, core, pl.ds(lax.rem(k, 2) * 2, 2)].reshape(512, 1024).astype(F32)
        rows = pl.ds(pl.multiple_of(k * 512, 512), 512)
        col_scale[rows, :] = jnp.sum(wide * wide, axis=1, keepdims=True) * scale
        return point_chunk(k, 0)

    lax.fori_loop(0, 2, early_chunk, 0)
    receive(there_up)
    handed[1] += [forward(part, 2, -1) for part in there]
    for copies in there_far:
        receive(copies)
    handed[1] += [forward(part, 2, 2) for part in there]
    receive_ring(late_ring)
    late_ring = around(late, 1)
    receive(handed[0])
    norms_line(1 - core)
    lax.fori_loop(2, 4, early_chunk, 0)
    receive(handed[1])
    lax.fori_loop(4, 8, point_chunk, 0)
    factor[...] = 64.0 / jnp.sqrt(jnp.sum(image[:count, 128:], axis=1, keepdims=True))
    receive_ring(late_ring)
    late_up = [send(part, 2, 0, 1) for part in late]
    late_down = [send(part, 2, 0, -1) for part in late]
    late_handed = [forward(part, 2, 0) for part in late]

    def land_chunk(j, _):
        rows = land[j // 8, lax.rem(j // 4, 2), lax.rem(j, 4)].reshape(256, 1024)
        cols = pl.ds(pl.multiple_of(j * 256, 256), 256)
        inner = dot_nt(land[:, core].reshape(half, 1024), rows)
        close = jnp.exp2(inner * (2.0 * scale) - (col_scale[...] + sq[:, cols]))
        kern[:, cols] = close
        image[:, :128] += close[:, :128] + close[:, 128:]
        csum[0, :, cols] += jnp.sum(close.reshape(half // 8, 8, 256), axis=0)
        return 0

    lax.fori_loop(0, 6, land_chunk, 0)
    receive(late_up + late_down)
    late_far = [send(late[0], 2, -1, 1), send(late[1], 2, 1, -1)]
    late_handed += [forward(part, 2, by) for part in late for by in (-1, 1)]
    lax.fori_loop(6, 12, land_chunk, 0)
    receive(late_far)
    late_handed += [forward(part, 2, 2) for part in late]
    lax.fori_loop(12, 16, land_chunk, 0)

    def swap(src, dst, sems, index):
        c = pltpu.make_async_remote_copy(
            src_ref=src, dst_ref=dst, send_sem=sems.at[0, index], recv_sem=sems.at[1, index],
            device_id=partner, device_id_type=MESH,
        )
        c.start()
        return c

    give = swap(csum.at[0], csum.at[1], c_sem, 0)
    col_scale[...] = 1.0 / jnp.sqrt(jnp.sum(image[:, :128], axis=1, keepdims=True))
    weights_copy(6, 0).wait()
    weights_copy(7, 1).wait()
    receive(late_handed)
    for c in sent + forwarded:
        c.wait_send()
    give.wait_recv()
    row_scale[...] = 1.0 / jnp.sqrt(jnp.sum(csum[0] + csum[1], axis=0, keepdims=True))
    give.wait_send()

    def low_piece(t, s, c):
        return land[s, c, pl.ds(2 * t, 2)].reshape(512, 1024)

    def up_piece(t, s, c):
        cols = pl.ds(pl.multiple_of(s * 2048 + c * 1024, 1024), 1024)
        return upper[pl.ds(pl.multiple_of(t * 512, 512), 512), cols]

    def half_product(piece, t, slot, c):
        rows = jnp.concatenate([piece(t, 0, c), piece(t, 1, c)], axis=1)
        return jnp.dot(rows, xs[slot, :, c].reshape(half, 256), preferred_element_type=F32)

    def scaled(r, b):
        cols = pl.ds(b * 1024, 1024)
        return (kern[r, cols] * col_scale[r, :] * row_scale[:, cols]).astype(BF16)

    def first_low(t, _):
        r = pl.ds(pl.multiple_of(t * 512, 512), 512)
        pieces = []
        for b in range(4):
            piece = scaled(r, b)
            land[b // 2, b % 2, pl.ds(2 * t, 2)] = piece.reshape(2, 4, 4, 16, 1024)
            pieces.append(piece)
        rows = jnp.concatenate(pieces, axis=1)
        image[r, :] = jnp.dot(rows, xs[0].reshape(2 * half, 256), preferred_element_type=F32)
        return 0

    def first_up(t, _):
        r = pl.ds(pl.multiple_of(1024 + t * 512, 512), 512)
        u = pl.ds(pl.multiple_of(t * 512, 512), 512)
        for b in range(4):
            upper[u, pl.ds(b * 1024, 1024)] = scaled(r, b)
        image[r, :] = jnp.dot(upper[u, :], xs[0].reshape(2 * half, 256), preferred_element_type=F32)
        return 0

    eye = lax.broadcasted_iota(jnp.int32, (256, 256), 0) == lax.broadcasted_iota(jnp.int32, (256, 256), 1)
    pending, gives = [], []
    for step in range(ITERS):
        last = step == ITERS - 1
        if step == 0:
            lax.fori_loop(0, 2, first_low, 0)
            lax.fori_loop(0, 2, first_up, 0)
        else:
            def product(piece, base, c, add):
                def tile(t, _):
                    r = pl.ds(pl.multiple_of(base + t * 512, 512), 512)
                    out = half_product(piece, t, step, c)
                    image[r, :] = image[r, :] + out if add else out
                    return 0

                lax.fori_loop(0, 2, tile, 0)

            product(low_piece, 0, core, False)
            product(up_piece, 1024, core, False)
            receive(gives)
            product(up_piece, 1024, 1 - core, True)
            if last:
                weights_in = pltpu.make_async_copy(weights_out, upper, w_sem.at[0])
                weights_in.start()
            product(low_piece, 0, 1 - core, True)
        hi, lo = split(image[...])
        gram = dot_tn(hi, jnp.concatenate([hi, lo], axis=1))
        cross = gram[:, 256:]
        grams[step, 0] = gram[:, :256] + cross + cross.T
        give = swap(grams.at[step, 0], grams.at[step, 1], g_sem, step)
        aug[:, 256:] = jnp.where(eye, 1.0, 0.0)
        give.wait_recv()
        aug[:, :256] = grams[step, 0] + grams[step, 1]
        pending.append(give)
        cholesky_inverse(aug, lower_t, inverse)
        ihi, ilo = split(inverse[...])
        stacked = jnp.concatenate([ihi, ilo, ihi], axis=1)
        if last:
            inverse_lam = 1.0 / jnp.sum(jnp.where(eye, lower_t[...], 0.0), axis=0, keepdims=True)
        gives = []
        target = 0 if last else step + 1
        for t in range(2):
            r = pl.ds(t * 1024, 1024)
            hi, lo = split(image[r, :])
            ortho = dot_nt(jnp.concatenate([hi, hi, lo], axis=1), stacked)
            if last:
                image[r, :] = ortho
                ortho = ortho * col_scale[r, :] * inverse_lam
            xs[target, t, core] = ortho.astype(BF16).reshape(4, 4, 4, 16, 256)
            part = xs.at[target, t, core]
            gives.append(swap(part, part, s_sem if last else x_sem, t))
        pending += gives

    index = at["z"] * 16 + at["y"] * 4 + at["x"]
    for s in range(2):
        rows = pl.ds(pl.multiple_of(s * 1024 + index * 16, 16), 16)
        own_out[16 * s : 16 * s + 16, :] = image[rows, :]
    weights_in.wait()
    for t in range(2):
        image[t * 512 : t * 512 + 512, :] = half_product(up_piece, t, 0, core)
    receive(gives)
    copies = []
    for t in range(2):
        r = pl.ds(t * 512, 512)
        image[r, :] = (image[r, :] + half_product(up_piece, t, 0, 1 - core)) * factor[r, :]
        copies.append(pltpu.make_async_copy(image.at[r, :], coords_out.at[r, :], o_sem.at[t]))
        copies[-1].start()
    for c in pending:
        c.wait_send()
    for c in copies:
        c.wait()


def deliver_kernel(own_ref, coords_ref, own_out, coords_out):
    own_out[...] = own_ref[...]
    coords_out[...] = coords_ref[...]


def body(landmarks, initial_basis, points):
    shard, width = landmarks.shape
    rank = initial_basis.shape[1]
    total = shard * 128
    half = total // 2
    count = points.shape[0]
    scale = LOG2E / (SPREAD * width)
    anywhere = pl.BlockSpec(memory_space=pl.ANY)
    vmem = pl.BlockSpec(memory_space=pltpu.VMEM)
    dma = pltpu.SemaphoreType.DMA
    results = (jax.ShapeDtypeStruct((shard, rank), F32), jax.ShapeDtypeStruct((count, rank), F32))

    own, coords, _ = pl.pallas_call(
        functools.partial(nystrom_kernel, scale),
        name="nystrom",
        out_shape=(*results, jax.ShapeDtypeStruct((count, total), BF16)),
        in_specs=[anywhere, anywhere, anywhere],
        out_specs=(vmem, anywhere, anywhere),
        scratch_shapes=[
            pltpu.VMEM((2, 2, 4, 4, 4, shard // 2, width), BF16),
            pltpu.VMEM((2, 2, 2, 4, 4, 4, shard // 2, rank), BF16),
            pltpu.VMEM((2, 4, 4, 4, 2, 128), F32),
            pltpu.VMEM((half, total), F32),
            pltpu.VMEM((count, total), BF16),
            pltpu.VMEM((half, rank), F32),
            pltpu.VMEM((1, total), F32),
            pltpu.VMEM((2, 8, total), F32),
            pltpu.VMEM((2, 2, rank, rank), F32),
            pltpu.VMEM((rank, 2 * rank), F32),
            pltpu.VMEM((rank, rank), F32),
            pltpu.VMEM((rank, rank), F32),
            pltpu.VMEM((half, 1), F32),
            pltpu.VMEM((1, total), F32),
            pltpu.VMEM((count, 1), F32),
            dma((5,)), dma((135,)), dma((135,)), dma((36,)), dma((36,)), dma((2,)),
            dma((2, 1)), dma((2, 2)), dma((2, 2)), dma((2, 2)), dma((2,)),
        ],
        compiler_params=pltpu.CompilerParams(
            collective_id=0, has_side_effects=True, vmem_limit_bytes=VMEM_LIMIT
        ),
    )(landmarks, initial_basis, points)
    return pl.pallas_call(
        deliver_kernel,
        name="deliver",
        out_shape=results,
        in_specs=[vmem, vmem],
        out_specs=(vmem, vmem),
    )(own, coords)


def solution(mesh):
    in_specs = (P(("grp", "row"), None), P(("grp", "row"), None), P(("grp", "row"), None))
    out_specs = (P(("grp", "row"), None), P(("grp", "row"), None))
    return jax.shard_map(body, mesh=mesh, in_specs=in_specs, out_specs=out_specs, check_vma=False)
```
